32 devices in a mesh: leaf: 8 (over z, x), vec: 4 (over y, core).
Axes of the slice: x: 2, y: 2, z: 4, core: 2. Of those that a mesh axis runs over, the one named last changes fastest.
Arguments:
- samples: bfloat16 [64, 32768], P('vec', 'leaf'), may hold values from -6 to 6
- coords: float32 [3, 32768], P(None, 'leaf'), may hold values from -4 to 4
- panel_area: float32 [32768], P('leaf'), may hold values from 0.05 to 0.5
- quad_weight: float32 [32768], P('leaf'), may hold values from 0.2 to 1
- leaf_basis: bfloat16 [128, 64, 256], P('leaf'), may hold values from -0.375 to 0.375
- transfer: bfloat16 [64, 2, 64, 64], P('leaf'), may hold values from -0.5 to 0.5
- coupling_fine: bfloat16 [128, 16, 64, 64], P('leaf'), may hold values from -0.1875 to 0.1875
- coupling_coarse: bfloat16 [64, 16, 64, 64], P('leaf'), may hold values from -0.1875 to 0.1875
- near_list: int32 [128, 16], P('leaf'), may hold values from 0 to 127, as said below
- send_fine: int32 [64, 32], P('leaf'), may hold values from 0 to 15
- send_coarse: int32 [64, 16], P('leaf'), may hold values from 0 to 7
- far_fine: int32 [128, 16], P('leaf'), may hold values from 0 to 255, as said below
- far_coarse: int32 [64, 16], P('leaf'), may hold values from 0 to 127, as said below
Outputs:
- sample_out: bfloat16 [64, 32768], P('vec', 'leaf')
- sample_gram: float32 [128, 64, 64], P('leaf', 'vec')
The draws below stay inside these ranges and needn't reach their ends.
Inputs may be any that keep to these rules, and one draw needn't show every extreme that they name: `near_list`: row g names 16 different leaves, each at most 16 leaves from g. `send_fine`: row e * 8 + d names clusters of device e, counted on e from 0; every slot carries one. `send_coarse`: row e * 8 + d names clusters of device e, counted on e from 0; every slot carries one. `far_fine`: the rows of one device's 16 leaves name each of the values 0 to 255 exactly once. `far_coarse`: the rows of one device's parents name each of the values 0 to 127 exactly once.
All inputs are finite; a program needn't handle non-finite values.
Results may differ from the reference program's by a relative error of at most 0.0085.
Values may be sent and summed in bfloat16 or wider, within the bound.
A program may use at most 64 MiB of HBM per device.

```python
import math
import jax
import jax.numpy as jnp
from jax import lax

LEAF = 256
K = 64
VECS = 64
NN = 16
HW = 16
NB = 16
LEAF_DEV = 16
LEAVES = 128
POINTS = 32768
PARENTS = 64
CAP0 = 32
CAP1 = 16
N_LEAF = 8


def draw_near_list(key, part):
    window_len = 2 * HW + 1
    offsets = jnp.arange(window_len, dtype=jnp.int32) - HW
    rank_bits = jax.random.randint(key, (LEAVES, window_len), 0, 1 << 20, dtype=jnp.int32)
    owner_leaf = jnp.arange(LEAVES, dtype=jnp.int32)[:, None]
    target = owner_leaf + offsets[None, :]
    inside = (target >= 0) & (target < LEAVES)
    scores = jnp.where(inside, rank_bits + (1 << 20), 0) * window_len + jnp.arange(window_len, dtype=jnp.int32)[None, :]
    top_scores, picked = lax.top_k(scores, NN)
    return jnp.take_along_axis(target, picked, axis=1).astype(jnp.int32)


def permuted_rows(key, per_device, width_nb):
    devices = LEAVES // LEAF_DEV
    device_keys = jax.random.split(key, devices)
    permuted = jax.vmap(lambda subkey: jax.random.permutation(subkey, per_device * width_nb))(device_keys)
    return permuted.reshape(devices * per_device, width_nb).astype(jnp.int32)


def draw_far_fine(key, part):
    return permuted_rows(jax.random.fold_in(key, 11), LEAF_DEV, NB)


def draw_far_coarse(key, part):
    return permuted_rows(jax.random.fold_in(key, 23), LEAF_DEV // 2, NB)


def touch_ends(values, key, least, largest):
    extent = values.shape
    place = [jax.random.randint(jax.random.fold_in(key, axis), (), 0, extent[axis]) for axis in range(len(extent))]
    values = values.at[tuple(place)].set(least)
    longest = extent.index(max(extent))
    place[longest] = (place[longest] + 1) % extent[longest]
    return values.at[tuple(place)].set(largest)


def block_levels(own_key, dims, cuts, least, largest):
    loudness, own = 1.0, jax.random.fold_in(own_key, 6)
    for dim, shards_of in cuts:
        steps = jnp.exp(jax.random.uniform(jax.random.fold_in(own, dim), (shards_of,), jnp.float32, least / len(cuts), largest / len(cuts)))
        loudness = loudness * jnp.repeat(steps, dims[dim] // shards_of).reshape([-1 if axis == dim else 1 for axis in range(len(dims))])
    return loudness


def centred(stream_key, shape, width, reach, pieces=(), held_as=jnp.bfloat16):
    result = width * jax.random.normal(stream_key, shape, jnp.float32)
    if pieces:
        result = result * block_levels(stream_key, shape, pieces, -0.22, 0.18)
    return jnp.clip(result, -reach, reach).astype(held_as)


def setup_inputs(seed: int = 0) -> dict:
    splits = jax.random.split(jax.random.key(seed), 14)
    return {
        "samples": centred(splits[0], (VECS, POINTS), 1.0, 6.0, ((0, 4), (1, 8))),
        "coords": centred(splits[1], (3, POINTS), 0.3, 4.0, ((1, 8),), jnp.float32),
        "panel_area": jnp.clip(jnp.exp(math.log(0.5) - 2.3025851 * jax.random.uniform(splits[2], (POINTS,), jnp.float32) ** block_levels(splits[2], (POINTS,), ((0, 8),), -0.2, 0.2)), 0.05, 0.5),
        "quad_weight": jnp.clip(0.2 + 0.8 * jax.random.uniform(splits[3], (POINTS,), jnp.float32) ** block_levels(splits[3], (POINTS,), ((0, 8),), -0.2, 0.2), 0.2, 1.0),
        "leaf_basis": centred(splits[4], (LEAVES, K, LEAF), LEAF ** -0.5, 0.375, ((0, 8),)),
        "transfer": centred(splits[5], (PARENTS, 2, K, K), (2 * K) ** -0.5, 0.5, ((0, 8),)),
        "coupling_fine": centred(splits[6], (LEAVES, NB, K, K), (NB * K) ** -0.5, 0.1875, ((0, 8),)),
        "coupling_coarse": centred(splits[7], (PARENTS, NB, K, K), (NB * K) ** -0.5, 0.1875, ((0, 8),)),
        "near_list": draw_near_list(jax.random.fold_in(splits[13], 71), 0),
        "send_fine": touch_ends(jax.random.randint(splits[9], (N_LEAF * N_LEAF, CAP0), 0, LEAF_DEV), jax.random.fold_in(splits[9], 1), 0, LEAF_DEV - 1).astype(jnp.int32),
        "send_coarse": touch_ends(jax.random.randint(splits[10], (N_LEAF * N_LEAF, CAP1), 0, LEAF_DEV // 2), jax.random.fold_in(splits[10], 1), 0, (LEAF_DEV // 2) - 1).astype(jnp.int32),
        "far_fine": draw_far_fine(jax.random.fold_in(splits[13], 71), 0),
        "far_coarse": draw_far_coarse(jax.random.fold_in(splits[13], 71), 0),
    }


four_pi = 4.0 * 3.141592653589793

def kernel_block(target, source):
    delta_x = target[0][:, None] - source[0][None, :]
    delta_y = target[1][:, None] - source[1][None, :]
    delta_z = target[2][:, None] - source[2][None, :]
    distance = delta_x * delta_x + delta_y * delta_y + delta_z * delta_z + source[3][None, :]
    return (source[4][None, :] / (four_pi * jnp.sqrt(distance))).astype(jnp.bfloat16)

def near_field(samples, geometry, near_list):
    leaves = near_list.shape[0]
    geo_all = geometry.reshape(5, leaves, LEAF)
    values = samples.reshape(samples.shape[0], leaves, LEAF)

    def leaf_group(indices):

        def one_leaf(index):
            chosen = near_list[index]
            src_geo = jnp.take(geo_all, chosen, axis=1)
            src_val = jnp.take(values, chosen, axis=1).astype(jnp.float32)
            target = jnp.take(geo_all[:3], index, axis=1)
            blocks = jax.vmap(kernel_block, (None, 1))(target, src_geo)
            return jnp.einsum('npq,vnq->vp', blocks.astype(jnp.float32), src_val)
        return jax.vmap(one_leaf)(indices)
    results = lax.map(leaf_group, jnp.arange(leaves, dtype=jnp.int32).reshape(-1, 8))
    return results.reshape(leaves, samples.shape[0], LEAF)

def partner_map(far_list, send_plan, per_device):
    slots = send_plan.shape[1]
    devices = far_list.shape[0] // per_device
    owner_dev = (jnp.arange(far_list.shape[0], dtype=jnp.int32) // per_device)[:, None]
    source = far_list // slots
    slot_index = far_list % slots
    local_index = send_plan[source * devices + owner_dev, slot_index]
    return (source * per_device + local_index).astype(jnp.int32)

def couple(tile_set, coef_table, partners, per_device):
    devices = partners.shape[0] // per_device
    width_nb = partners.shape[1]
    tile_set = tile_set.reshape(devices, per_device, width_nb, K, K)
    partners = partners.reshape(devices, per_device, width_nb)

    def one_device(operands):
        tiles, chosen = operands
        picked = coef_table[chosen].astype(jnp.float32)
        return jnp.einsum('ibkl,ibvl->ivk', tiles.astype(jnp.float32), picked)
    results = lax.map(one_device, (tile_set, partners))
    return results.reshape(devices * per_device, coef_table.shape[1], K)

def reference(samples, coords, panel_area, quad_weight, leaf_basis, transfer, coupling_fine, coupling_coarse, near_list, send_fine, send_coarse, far_fine, far_coarse):
    vectors = samples.shape[0]
    leaves = leaf_basis.shape[0]
    geometry = jnp.concatenate([coords, panel_area[None, :], quad_weight[None, :]], axis=0)
    near_part = near_field(samples, geometry, near_list)
    local_rows = samples.reshape(vectors, leaves, LEAF).astype(jnp.float32)
    fine_coef = jnp.einsum('ikp,vip->ivk', leaf_basis.astype(jnp.float32), local_rows).astype(jnp.bfloat16)
    coarse_coef = jnp.einsum('mskl,msvk->mvl', transfer.astype(jnp.float32), fine_coef.reshape(-1, 2, vectors, K).astype(jnp.float32)).astype(jnp.bfloat16)
    fine_partners = partner_map(far_fine, send_fine, LEAF_DEV)
    coarse_partners = partner_map(far_coarse, send_coarse, LEAF_DEV // 2)
    field_fine = couple(coupling_fine, fine_coef, fine_partners, LEAF_DEV)
    field_coarse = couple(coupling_coarse, coarse_coef, coarse_partners, LEAF_DEV // 2).astype(jnp.bfloat16)
    pushed = jnp.einsum('mskl,mvl->msvk', transfer.astype(jnp.float32), field_coarse.astype(jnp.float32))
    local_field = (field_fine + pushed.reshape(leaves, vectors, K)).astype(jnp.bfloat16)
    far_part = jnp.einsum('ikp,ivk->vip', leaf_basis.astype(jnp.float32), local_field.astype(jnp.float32))
    sample_out = (jnp.transpose(near_part, (1, 0, 2)) + far_part).reshape(vectors, leaves * LEAF).astype(jnp.bfloat16)
    shaped = sample_out.reshape(vectors, leaves, LEAF).astype(jnp.float32)
    sample_gram = jnp.einsum('aip,cip->iac', shaped, shaped) * (1.0 / LEAF)
    return (sample_out, sample_gram)
```

```python
import functools
import jax
import jax.numpy as jnp
from jax import lax
from jax.experimental import pallas as pl
from jax.experimental.pallas import tpu as pltpu
from jax.sharding import PartitionSpec as P

four_pi = 4.0 * 3.141592653589793
NT = (((1,), (1,)), ((), ()))
MESH = pl.DeviceIdType.MESH
LAG = 4


def pieces(block):
    first = block.astype(jnp.bfloat16).astype(jnp.float32)
    rest = block - first
    second = rest.astype(jnp.bfloat16).astype(jnp.float32)
    return first, second, rest - second


def main_kernel(
    near_ref, farf_ref, farc_ref,
    coords_ref, area_ref, weight_ref, sam_ref, sendf_ref, sendc_ref, transfer_ref, basis_ref, cf_hbm, cc_hbm,
    out_ref, gram_ref,
    geo_all, wvec, table, got, got_smem, coef_pk, fine_all, coarse_all, cf_ref, cc_ref,
    yfeat, xfeat, near_all, rows_all, gram_out,
    geo_send, geo_recv, geo_fsend, geo_frecv, sam_send, sam_recv, sam_fsend, sam_frecv,
    table_send, table_recv, coef_send, coef_recv, coef_fsend, coef_frecv,
    rows_send, rows_recv, out_send, out_recv, gram_send, gram_recv, local_sem,
):
    leaf_dev, basis_rank, leaf_pts = basis_ref.shape
    vec_dev = sam_ref.shape[0]
    parents = leaf_dev // 2
    cap0, cap1 = sendf_ref.shape[1], sendc_ref.shape[1]
    nb = farf_ref.shape[1]
    nbc = farc_ref.shape[1]
    nn = near_ref.shape[1]
    half_leaves, half_parents = leaf_dev // 2, parents // 2
    both = 2 * vec_dev
    devices, vecs = lax.axis_size("leaf"), lax.axis_size("vec")
    groups = vecs // 2
    me, row = lax.axis_index("leaf"), lax.axis_index("vec")
    h, g = lax.rem(row, 2), lax.div(row, 2)
    partner = {"vec": row + 1 - 2 * h}
    first_leaf, first_parent = h * half_leaves, h * half_parents

    def leaf_peer(step):
        return {"leaf": lax.rem(me + step, devices)}

    def group_peer(step):
        return {"vec": lax.rem(g + step, groups) * 2 + h}

    def remote(src, dst, send, recv, peer):
        return pltpu.make_async_remote_copy(
            src_ref=src, dst_ref=dst, send_sem=send, recv_sem=recv,
            device_id=peer, device_id_type=MESH,
        )

    def cut(leaf):
        return pl.ds(pl.multiple_of(leaf * leaf_pts, leaf_pts), leaf_pts)

    def nt(a, b):
        return lax.dot_general(a, b, NT, preferred_element_type=jnp.float32)

    barrier = pltpu.get_barrier_semaphore()

    def greet(step, carry):
        pl.semaphore_signal(barrier, inc=1, device_id=leaf_peer(step), device_id_type=MESH)
        return carry

    lax.fori_loop(1, devices, greet, 0)
    pl.semaphore_signal(barrier, inc=1, device_id=partner, device_id_type=MESH)
    for step in range(1, groups):
        pl.semaphore_signal(barrier, inc=1, device_id=group_peer(step), device_id_type=MESH)

    load_fine = pltpu.make_async_copy(cf_hbm.at[pl.ds(first_leaf, half_leaves)], cf_ref, local_sem.at[0])
    load_coarse = pltpu.make_async_copy(cc_hbm.at[pl.ds(first_parent, half_parents)], cc_ref, local_sem.at[1])
    load_fine.start()
    load_coarse.start()

    def own(leaf, carry):
        xyz = coords_ref[:, cut(leaf)]
        norm = jnp.sum(xyz * xyz, axis=0, keepdims=True) + area_ref[:, cut(leaf)]
        geo_all[leaf_dev + leaf] = jnp.concatenate([xyz, norm], axis=0)
        weight = weight_ref[:, cut(leaf)] * (1.0 / four_pi)
        scaled = sam_ref[:, cut(leaf)].astype(jnp.float32) * weight
        wvec[leaf_dev + leaf, h] = scaled.astype(jnp.bfloat16)
        return carry

    lax.fori_loop(0, leaf_dev, own, 0, unroll=4)
    table[...] = jnp.zeros_like(table)

    def fill(d, carry):
        table[d, 0:1, 0:cap0] = sendf_ref[pl.ds(d, 1), :]
        table[d, 1:2, 0:cap1] = sendc_ref[pl.ds(d, 1), :]
        return carry

    lax.fori_loop(0, devices, fill, 0)
    got[me] = table[me]
    pl.semaphore_wait(barrier, devices - 1 + 1 + groups - 1)

    def sides(run):
        @pl.when(me < devices - 1)
        def _():
            run(0, leaf_peer(1))

        @pl.when(me > 0)
        def _():
            run(1, leaf_peer(devices - 1))

    def geo_copy(side, peer):
        src = geo_all.at[pl.ds(leaf_dev + first_leaf, half_leaves)]
        dst = geo_all.at[pl.ds(side * 2 * leaf_dev + first_leaf, half_leaves)]
        return remote(src, dst, geo_send.at[side], geo_recv.at[side], peer)

    def geo_forward(side):
        part = geo_all.at[pl.ds(side * 2 * leaf_dev + first_leaf, half_leaves)]
        return remote(part, part, geo_fsend.at[side], geo_frecv.at[side], partner)

    def sam_copy(side, peer):
        src = wvec.at[pl.ds(leaf_dev, leaf_dev), h]
        dst = wvec.at[pl.ds(side * 2 * leaf_dev, leaf_dev), h]
        return remote(src, dst, sam_send.at[side], sam_recv.at[side], peer)

    def sam_forward(part):
        block = wvec.at[pl.ds(part * leaf_dev, leaf_dev), h]
        return remote(block, block, sam_fsend.at[part], sam_frecv.at[part], partner)

    def table_copy(step):
        peer = lax.rem(me + step, devices)
        return remote(table.at[peer], got.at[me], table_send.at[step], table_recv.at[step], {"leaf": peer})

    def coef_copy(step):
        part = coef_pk.at[me, :, h]
        return remote(part, part, coef_send.at[step], coef_recv.at[step], leaf_peer(step))

    def coef_forward(step):
        part = coef_pk.at[lax.rem(me - step + devices, devices), :, h]
        return remote(part, part, coef_fsend.at[step], coef_frecv.at[step], partner)

    sides(lambda side, peer: geo_copy(side, peer).start())
    sides(lambda side, peer: sam_copy(side, peer).start())
    sam_forward(1).start()

    def start_table(step, carry):
        table_copy(step).start()
        return carry

    lax.fori_loop(1, devices, start_table, 0)

    blank = jnp.zeros((basis_rank, leaf_pts), jnp.bfloat16)
    packed = []
    for m in range(parents):
        left = jnp.concatenate([basis_ref[2 * m], blank], axis=0)
        right = jnp.concatenate([blank, basis_ref[2 * m + 1]], axis=0)
        coef = nt(sam_ref[:, cut(2 * m)], left) + nt(sam_ref[:, cut(2 * m + 1)], right)
        coef = coef.astype(jnp.bfloat16)
        coef_pk[me, m, h] = coef
        packed.append(coef)
    coarse = []
    for m in range(parents):
        both_children = transfer_ref[m].reshape(2 * basis_rank, basis_rank)
        coarse.append(jnp.dot(packed[m], both_children, preferred_element_type=jnp.float32))
    for m in range(half_parents):
        pair = jnp.concatenate([coarse[2 * m], coarse[2 * m + 1]], axis=1)
        coef_pk[me, parents + m, h] = pair.astype(jnp.bfloat16)

    def prepare(part):
        def source(leaf, carry):
            geo = geo_all[part * leaf_dev + leaf]
            ones = jnp.ones((1, leaf_pts), jnp.float32)
            rows = jnp.concatenate([geo, ones, jnp.zeros((3, leaf_pts), jnp.float32)], axis=0)
            y1, y2, y3 = pieces(rows)
            rows = jnp.concatenate([y1, y1, y1, y2, y2, y3], axis=0)
            yfeat[part * leaf_dev + leaf] = rows.T.astype(jnp.bfloat16)
            return carry

        lax.fori_loop(0, leaf_dev, source, 0, unroll=4)

    prepare(1)

    def target(leaf, carry):
        xyz = geo_all[leaf_dev + first_leaf + leaf][0:3]
        norm = jnp.sum(xyz * xyz, axis=0, keepdims=True)
        x8 = jnp.concatenate(
            [-2.0 * xyz, jnp.ones_like(norm), norm, jnp.zeros_like(xyz)], axis=0
        )
        x1, x2, x3 = pieces(x8)
        features = jnp.concatenate([x1, x2, x3, x1, x2, x1], axis=0).astype(jnp.bfloat16)
        xfeat[0, leaf] = features
        xfeat[1, leaf] = features
        return carry

    lax.fori_loop(0, half_leaves, target, 0, unroll=2)

    def start_coef(step, carry):
        coef_copy(step).start()
        return carry

    def incoming(run):
        @pl.when(me > 0)
        def _():
            run(0)

        @pl.when(me < devices - 1)
        def _():
            run(1)

    def pass_geo(side):
        geo_copy(side, leaf_peer(0)).wait_recv()
        geo_forward(side).start()

    def use_geo(side):
        geo_forward(side).wait_recv()
        prepare(2 * side)

    def pass_sam(side):
        sam_copy(side, leaf_peer(0)).wait_recv()
        sam_forward(2 * side).start()

    incoming(pass_geo)
    incoming(use_geo)
    coef_forward(0).start()
    lax.fori_loop(1, devices, start_coef, 0)
    incoming(pass_sam)
    sam_forward(1).wait_recv()
    incoming(lambda side: sam_forward(2 * side).wait_recv())

    def near_leaf(leaf, carry):
        features = [xfeat[0, leaf], xfeat[1, leaf]]
        total = [None, None]
        base = (me - 1) * leaf_dev
        picked = [
            jnp.clip(near_ref[first_leaf + leaf, n] - base, 0, 3 * leaf_dev - 1) for n in range(nn)
        ]
        dists = {}
        for n in range(nn + LAG):
            if n < nn:
                dists[n] = jnp.dot(yfeat[picked[n]], features[n % 2], preferred_element_type=jnp.float32)
            m = n - LAG
            if m >= 0:
                block = lax.rsqrt(dists.pop(m).astype(jnp.bfloat16))
                values = wvec[picked[m]].reshape(both, leaf_pts)
                term = jnp.dot(values, block, preferred_element_type=jnp.float32)
                total[m % 2] = term if total[m % 2] is None else total[m % 2] + term
        near_all[0, leaf] = total[0]
        near_all[1, leaf] = total[1]
        return carry

    lax.fori_loop(0, half_leaves - 2, near_leaf, 0)

    def pass_coef(step, carry):
        coef_copy(step).wait_recv()
        coef_forward(step).start()
        return carry

    lax.fori_loop(1, devices, pass_coef, 0)
    lax.fori_loop(half_leaves - 2, half_leaves, near_leaf, 0)

    coef_forward(0).wait_recv()

    def finish(step, carry):
        table_copy(step).wait()
        coef_copy(step).wait_send()
        coef_forward(step).wait_recv()
        return carry

    lax.fori_loop(1, devices, finish, 0)
    to_smem = pltpu.make_async_copy(got, got_smem, local_sem.at[2])
    to_smem.start()

    def unpack(d, carry):
        for m in range(parents):
            pair = coef_pk[d, m].reshape(both, 2 * basis_rank)
            fine_all[d * leaf_dev + 2 * m] = pair[:, :basis_rank]
            fine_all[d * leaf_dev + 2 * m + 1] = pair[:, basis_rank:]
        for m in range(half_parents):
            pair = coef_pk[d, parents + m].reshape(both, 2 * basis_rank)
            coarse_all[d * parents + 2 * m] = pair[:, :basis_rank]
            coarse_all[d * parents + 2 * m + 1] = pair[:, basis_rank:]
        return carry

    lax.fori_loop(0, devices, unpack, 0)
    load_fine.wait()
    load_coarse.wait()
    to_smem.wait()

    def fine_term(leaf, b):
        slot = farf_ref[first_leaf + leaf, b]
        source = lax.div(slot, cap0)
        index = source * leaf_dev + got_smem[source, 0, lax.rem(slot, cap0)]
        return nt(fine_all[index], cf_ref[leaf, b])

    def coarse_term(m, b):
        slot = farc_ref[first_parent + m, b]
        source = lax.div(slot, cap1)
        index = source * parents + got_smem[source, 1, lax.rem(slot, cap1)]
        return nt(coarse_all[index], cc_ref[m, b])

    def rows_copy(m, step):
        part = rows_all.at[g, :, :, pl.ds(pl.multiple_of(m * 2 * leaf_pts, 2 * leaf_pts), 2 * leaf_pts)]
        return remote(part, part, rows_send.at[step, m], rows_recv.at[step, m], group_peer(step))

    def out_copy(m):
        columns = pl.ds(pl.multiple_of(m * 2 * leaf_pts, 2 * leaf_pts), 2 * leaf_pts)
        start = (first_leaf + 2 * m) * leaf_pts
        there = pl.ds(pl.multiple_of(start, 2 * leaf_pts), 2 * leaf_pts)
        return remote(
            rows_all.at[g, 1 - h, :, columns], out_ref.at[:, there], out_send.at[m], out_recv.at[m], partner
        )

    coarse_field = []
    for m in range(half_parents):
        field = coarse_term(m, 0)
        for b in range(1, nbc):
            field = field + coarse_term(m, b)
        coarse_field.append(field.astype(jnp.bfloat16))
    locals_ = []
    for leaf in range(half_leaves):
        field = nt(coarse_field[leaf // 2], transfer_ref[first_parent + leaf // 2, leaf % 2])
        for b in range(nb):
            field = field + fine_term(leaf, b)
        locals_.append(field.astype(jnp.bfloat16))
    for m in range(half_parents):
        for leaf in (2 * m, 2 * m + 1):
            far = jnp.dot(locals_[leaf], basis_ref[first_leaf + leaf], preferred_element_type=jnp.float32)
            result = (near_all[0, leaf] + near_all[1, leaf] + far).astype(out_ref.dtype)
            result = result.reshape(2, vec_dev, leaf_pts)
            rows_all[g, :, :, cut(leaf)] = result
        for step in range(1, groups):
            rows_copy(m, step).start()
        out_copy(m).start()

    for leaf in range(half_leaves):
        out_ref[:, cut(first_leaf + leaf)] = rows_all[g, h, :, cut(leaf)]

    def gram_pair(m, carry):
        for step in range(1, groups):
            rows_copy(m, step).wait()
        for s in range(2):
            leaf = 2 * m + s
            everyone = rows_all[:, :, :, cut(leaf)].reshape(vecs * vec_dev, leaf_pts)
            gram_ref[first_leaf + leaf] = nt(rows_all[g, h, :, cut(leaf)], everyone) * (1.0 / leaf_pts)
            gram_out[leaf] = nt(rows_all[g, 1 - h, :, cut(leaf)], everyone) * (1.0 / leaf_pts)
        return carry

    lax.fori_loop(0, half_parents, gram_pair, 0)
    gram_copy = remote(
        gram_out, gram_ref.at[pl.ds(first_leaf, half_leaves)], gram_send.at[0], gram_recv.at[0], partner
    )
    gram_copy.start()

    sides(lambda side, peer: geo_copy(side, peer).wait_send())
    sides(lambda side, peer: sam_copy(side, peer).wait_send())
    incoming(lambda side: geo_forward(side).wait_send())
    incoming(lambda side: sam_forward(2 * side).wait_send())
    sam_forward(1).wait_send()

    def drain(step, carry):
        coef_forward(step).wait_send()
        return carry

    lax.fori_loop(0, devices, drain, 0)
    for m in range(half_parents):
        out_copy(m).wait()
    gram_copy.wait()


def per_device(
    samples, coords, panel_area, quad_weight, leaf_basis, transfer,
    coupling_fine, coupling_coarse, near_list, send_fine, send_coarse, far_fine, far_coarse,
):
    vec_dev, points = samples.shape
    leaf_dev, basis_rank, leaf_pts = leaf_basis.shape
    parents, half = leaf_dev // 2, leaf_dev // 2
    devices, vecs = lax.axis_size("leaf"), lax.axis_size("vec")
    groups, both = vecs // 2, 2 * vec_dev
    nb, nbc = coupling_fine.shape[1], coupling_coarse.shape[1]
    smem = pl.BlockSpec(memory_space=pltpu.SMEM)
    vmem = pl.BlockSpec(memory_space=pltpu.VMEM)
    hbm = pl.BlockSpec(memory_space=pl.ANY)
    bf16, f32 = jnp.bfloat16, jnp.float32
    dma = pltpu.SemaphoreType.DMA
    sample_out, gram = pl.pallas_call(
        main_kernel,
        out_shape=(
            jax.ShapeDtypeStruct((vec_dev, points), bf16),
            jax.ShapeDtypeStruct((leaf_dev, vec_dev, vecs * vec_dev), f32),
        ),
        in_specs=[smem] * 3 + [vmem] * 8 + [hbm] * 2,
        out_specs=(vmem, vmem),
        scratch_shapes=[
            pltpu.VMEM((3 * leaf_dev, 4, leaf_pts), f32),
            pltpu.VMEM((3 * leaf_dev, 2, vec_dev, leaf_pts), bf16),
            pltpu.VMEM((devices, 2, 128), jnp.int32),
            pltpu.VMEM((devices, 2, 128), jnp.int32),
            pltpu.SMEM((devices, 2, 128), jnp.int32),
            pltpu.VMEM((devices, parents + parents // 2, 2, vec_dev, 2 * basis_rank), bf16),
            pltpu.VMEM((devices * leaf_dev, both, basis_rank), bf16),
            pltpu.VMEM((devices * parents, both, basis_rank), bf16),
            pltpu.VMEM((half, nb, basis_rank, basis_rank), bf16),
            pltpu.VMEM((half // 2, nbc, basis_rank, basis_rank), bf16),
            pltpu.VMEM((3 * leaf_dev, leaf_pts, 48), bf16),
            pltpu.VMEM((2, half, 48, leaf_pts), bf16),
            pltpu.VMEM((2, half, both, leaf_pts), f32),
            pltpu.VMEM((groups, 2, vec_dev, half * leaf_pts), bf16),
            pltpu.VMEM((half, vec_dev, vecs * vec_dev), f32),
            dma((2,)), dma((2,)), dma((2,)), dma((2,)),
            dma((2,)), dma((2,)), dma((3,)), dma((3,)),
            dma((devices,)), dma((devices,)),
            dma((devices,)), dma((devices,)), dma((devices,)), dma((devices,)),
            dma((groups, half // 2)), dma((groups, half // 2)),
            dma((half // 2,)), dma((half // 2,)),
            dma((1,)), dma((1,)),
            dma((3,)),
        ],
        compiler_params=pltpu.CompilerParams(
            vmem_limit_bytes=56 * 1024 * 1024, collective_id=0, has_side_effects=True
        ),
    )(
        near_list, far_fine, far_coarse,
        coords, panel_area[None, :], quad_weight[None, :], samples, send_fine, send_coarse,
        transfer, leaf_basis, coupling_fine, coupling_coarse,
    )
    return sample_out, gram


def solution(mesh):
    return jax.shard_map(
        per_device,
        mesh=mesh,
        in_specs=(
            P("vec", "leaf"), P(None, "leaf"), P("leaf"), P("leaf"),
            P("leaf", None, None), P("leaf", None, None, None),
            P("leaf", None, None, None), P("leaf", None, None, None),
            P("leaf", None), P("leaf", None), P("leaf", None), P("leaf", None), P("leaf", None),
        ),
        out_specs=(P("vec", "leaf"), P("leaf", "vec", None)),
        check_vma=False,
    )
```

```python
import functools
import jax
import jax.numpy as jnp
from jax import lax
from jax.experimental import pallas as pl
from jax.experimental.pallas import tpu as pltpu
from jax.sharding import PartitionSpec as P

four_pi = 4.0 * 3.141592653589793
NT = (((1,), (1,)), ((), ()))
MESH = pl.DeviceIdType.MESH
LAG = 4
CHUNKS = 4
MATE_AT, FAR_AT = 1, 2


def pieces(block):
    first = block.astype(jnp.bfloat16).astype(jnp.float32)
    rest = block - first
    second = rest.astype(jnp.bfloat16).astype(jnp.float32)
    return first, second, rest - second


def main_kernel(
    near_hbm, farf_hbm, farc_hbm,
    coords_hbm, area_hbm, weight_hbm, sam_hbm, sendf_hbm, sendc_hbm, transfer_hbm, basis_hbm, cf_hbm, cc_hbm,
    out_ref, gram_ref,
    near_ref, farf_ref, farc_ref,
    coords_ref, area_ref, weight_ref, sam_ref, sendf_ref, sendc_ref, transfer_ref, basis_ref,
    geo_all, wvec, table, got, got_smem, coef_pk, fine_all, coarse_all, cf_ref, cc_ref,
    yfeat, xfeat, near_all, local_ref, rows_all, gram_out,
    geo_send, geo_recv, geo_fsend, geo_frecv, sam_send, sam_recv, sam_fsend, sam_frecv, own_send, own_recv,
    table_send, table_recv, coef_send, coef_recv, mate_send, mate_recv, coef_fsend, coef_frecv,
    rows_send, rows_recv, out_send, out_recv, gram_send, gram_recv, local_sem,
):
    leaf_dev, basis_rank, leaf_pts = basis_ref.shape
    vec_dev = sam_ref.shape[0]
    parents = leaf_dev // 2
    cap0, cap1 = sendf_ref.shape[1], sendc_ref.shape[1]
    nb = farf_ref.shape[1]
    nbc = farc_ref.shape[1]
    nn = near_ref.shape[1]
    half_leaves, half_parents = leaf_dev // 2, parents // 2
    both = 2 * vec_dev
    chunk = leaf_dev // CHUNKS
    devices, vecs = lax.axis_size("leaf"), lax.axis_size("vec")
    groups, columns = vecs // 2, devices // 2
    me, row = lax.axis_index("leaf"), lax.axis_index("vec")
    h, g = lax.rem(row, 2), lax.div(row, 2)
    partner = {"vec": row + 1 - 2 * h}
    first_leaf, first_parent = h * half_leaves, h * half_parents

    def leaf_peer(step):
        return {"leaf": lax.rem(me + step, devices)}

    def group_peer(step):
        return {"vec": lax.rem(g + step, groups) * 2 + h}

    def remote(src, dst, send, recv, peer):
        return pltpu.make_async_remote_copy(
            src_ref=src, dst_ref=dst, send_sem=send, recv_sem=recv,
            device_id=peer, device_id_type=MESH,
        )

    def cut(leaf):
        return pl.ds(pl.multiple_of(leaf * leaf_pts, leaf_pts), leaf_pts)

    def nt(a, b):
        return lax.dot_general(a, b, NT, preferred_element_type=jnp.float32)

    loads = [
        pltpu.make_async_copy(src, dst, local_sem.at[n])
        for n, (src, dst) in enumerate([
            (coords_hbm, coords_ref), (area_hbm, area_ref), (weight_hbm, weight_ref), (sam_hbm, sam_ref),
            (sendf_hbm, sendf_ref), (sendc_hbm, sendc_ref), (basis_hbm, basis_ref), (transfer_hbm, transfer_ref),
            (cf_hbm.at[pl.ds(first_leaf, half_leaves)], cf_ref),
            (cc_hbm.at[pl.ds(first_parent, half_parents)], cc_ref),
            (near_hbm, near_ref), (farf_hbm, farf_ref), (farc_hbm, farc_ref),
        ])
    ]
    for load in loads:
        load.start()
    barrier = pltpu.get_barrier_semaphore()

    def greet(step, carry):
        pl.semaphore_signal(barrier, inc=1, device_id=leaf_peer(step), device_id_type=MESH)
        return carry

    lax.fori_loop(1, devices, greet, 0)
    pl.semaphore_signal(barrier, inc=1, device_id=partner, device_id_type=MESH)
    for step in range(1, groups):
        pl.semaphore_signal(barrier, inc=1, device_id=group_peer(step), device_id_type=MESH)

    for load in loads[:6]:
        load.wait()

    def own(leaf, carry):
        xyz = coords_ref[:, cut(leaf)]
        norm = jnp.sum(xyz * xyz, axis=0, keepdims=True) + area_ref[:, cut(leaf)]
        geo_all[leaf_dev + leaf] = jnp.concatenate([xyz, norm], axis=0)
        weight = weight_ref[:, cut(leaf)] * (1.0 / four_pi)
        scaled = sam_ref[:, cut(leaf)].astype(jnp.float32) * weight
        wvec[leaf_dev + leaf, h] = scaled.astype(jnp.bfloat16)
        return carry

    lax.fori_loop(0, leaf_dev, own, 0, unroll=4)
    table[...] = jnp.zeros_like(table)

    def fill(d, carry):
        table[d, 0:1, 0:cap0] = sendf_ref[pl.ds(d, 1), :]
        table[d, 1:2, 0:cap1] = sendc_ref[pl.ds(d, 1), :]
        return carry

    lax.fori_loop(0, devices, fill, 0)
    got[me] = table[me]
    pl.semaphore_wait(barrier, devices - 1 + 1 + groups - 1)

    odd = lax.rem(me, 2)
    mate = {"leaf": me + 1 - 2 * odd}
    from_mate, from_relay = 2 * (1 - odd), 2 * odd
    onward = {"leaf": me + 2 - 4 * odd}
    sends_on = jnp.where(odd == 0, me + 2 < devices, me >= 2)
    gets_relay = jnp.where(odd == 0, me >= 2, me + 2 < devices)

    def geo_part(part):
        return geo_all.at[pl.ds(part * leaf_dev + first_leaf, half_leaves)]

    def sam_part(part, c):
        return wvec.at[pl.ds(part * leaf_dev + c * chunk, chunk), h]

    def geo_copy():
        return remote(geo_part(1), geo_part(from_relay), geo_send.at[0], geo_recv.at[0], mate)

    def geo_relay():
        return remote(geo_part(from_mate), geo_part(from_relay), geo_send.at[1], geo_recv.at[1], onward)

    def geo_forward(part, n):
        return remote(geo_part(part), geo_part(part), geo_fsend.at[n], geo_frecv.at[n], partner)

    def sam_copy(c):
        return remote(sam_part(1, c), sam_part(from_relay, c), sam_send.at[0, c], sam_recv.at[0, c], mate)

    def sam_relay(c):
        return remote(sam_part(from_mate, c), sam_part(from_relay, c), sam_send.at[1, c], sam_recv.at[1, c], onward)

    def sam_forward(part, n, c):
        block = sam_part(part, c)
        return remote(block, block, sam_fsend.at[n, c], sam_frecv.at[n, c], partner)

    def own_forward():
        block = wvec.at[pl.ds(leaf_dev, leaf_dev), h]
        return remote(block, block, own_send.at[0], own_recv.at[0], partner)

    def table_copy(step):
        peer = lax.rem(me + step, devices)
        return remote(table.at[peer], got.at[me], table_send.at[step], table_recv.at[step], {"leaf": peer})

    def same(step):
        return lax.rem(me + 2 * step, devices)

    def block_from(step):
        return lax.rem(me - 2 * step + devices, devices)

    def mate_block(step):
        return lax.rem(me + 1 - 2 * odd - 2 * step + devices, devices)

    def coef_copy(step):
        part = coef_pk.at[me, :, h]
        return remote(part, part, coef_send.at[step], coef_recv.at[step], {"leaf": same(step)})

    def coef_across(step):
        part = coef_pk.at[block_from(step), :, h]
        return remote(part, part, mate_send.at[step], mate_recv.at[step], mate)

    def coef_forward(step):
        part = coef_pk.at[block_from(step), :, h]
        return remote(part, part, coef_fsend.at[0, step], coef_frecv.at[0, step], partner)

    def mate_forward(step):
        part = coef_pk.at[mate_block(step), :, h]
        return remote(part, part, coef_fsend.at[1, step], coef_frecv.at[1, step], partner)

    geo_copy().start()
    for c in range(CHUNKS):
        sam_copy(c).start()
    own_forward().start()

    def start_table(step, carry):
        table_copy(step).start()
        return carry

    lax.fori_loop(1, devices, start_table, 0)

    loads[6].wait()
    loads[7].wait()
    blank = jnp.zeros((basis_rank, leaf_pts), jnp.bfloat16)
    packed = []
    for m in range(parents):
        left = jnp.concatenate([basis_ref[2 * m], blank], axis=0)
        right = jnp.concatenate([blank, basis_ref[2 * m + 1]], axis=0)
        coef = nt(sam_ref[:, cut(2 * m)], left) + nt(sam_ref[:, cut(2 * m + 1)], right)
        coef = coef.astype(jnp.bfloat16)
        coef_pk[me, m, h] = coef
        packed.append(coef)
    coarse = []
    for m in range(parents):
        both_children = transfer_ref[m].reshape(2 * basis_rank, basis_rank)
        coarse.append(jnp.dot(packed[m], both_children, preferred_element_type=jnp.float32))
    for m in range(half_parents):
        pair = jnp.concatenate([coarse[2 * m], coarse[2 * m + 1]], axis=1)
        coef_pk[me, parents + m, h] = pair.astype(jnp.bfloat16)

    def start_coef(step, carry):
        coef_copy(step).start()
        return carry

    lax.fori_loop(1, columns, start_coef, 0)
    coef_across(0).start()
    coef_forward(0).start()

    def prepare(part):
        def source(leaf, carry):
            geo = geo_all[part * leaf_dev + leaf]
            ones = jnp.ones((1, leaf_pts), jnp.float32)
            rows = jnp.concatenate([geo, ones, jnp.zeros((3, leaf_pts), jnp.float32)], axis=0)
            y1, y2, y3 = pieces(rows)
            rows = jnp.concatenate([y1, y1, y1, y2, y2, y3], axis=0)
            yfeat[part * leaf_dev + leaf] = rows.T.astype(jnp.bfloat16)
            return carry

        lax.fori_loop(0, leaf_dev, source, 0, unroll=4)

    prepare(1)

    def target(leaf, carry):
        xyz = geo_all[leaf_dev + first_leaf + leaf][0:3]
        norm = jnp.sum(xyz * xyz, axis=0, keepdims=True)
        x8 = jnp.concatenate(
            [-2.0 * xyz, jnp.ones_like(norm), norm, jnp.zeros_like(xyz)], axis=0
        )
        x1, x2, x3 = pieces(x8)
        features = jnp.concatenate([x1, x2, x3, x1, x2, x1], axis=0).astype(jnp.bfloat16)
        xfeat[0, leaf] = features
        xfeat[1, leaf] = features
        return carry

    lax.fori_loop(0, half_leaves, target, 0, unroll=2)

    def pass_coef(step, carry):
        coef_copy(step).wait_recv()
        coef_across(step).start()
        coef_forward(step).start()
        return carry

    def pass_mate_sam(c):
        sam_copy(c).wait_recv()

        @pl.when(sends_on)
        def _():
            sam_relay(c).start()

        sam_forward(from_mate, 0, c).start()

    geo_copy().wait_recv()

    @pl.when(sends_on)
    def _():
        geo_relay().start()

    geo_forward(from_mate, 0).start()
    pass_mate_sam(0)
    geo_forward(from_mate, 0).wait_recv()
    prepare(from_mate)
    for c in range(1, CHUNKS):
        pass_mate_sam(c)
    lax.fori_loop(1, columns, pass_coef, 0)

    @pl.when(gets_relay)
    def _():
        geo_relay().wait_recv()
        geo_forward(from_relay, 1).start()
        geo_forward(from_relay, 1).wait_recv()
        prepare(from_relay)
        for c in range(CHUNKS):
            sam_relay(c).wait_recv()
            sam_forward(from_relay, 1, c).start()

    own_forward().wait_recv()
    for c in range(CHUNKS):
        sam_forward(from_mate, 0, c).wait_recv()

    @pl.when(gets_relay)
    def _():
        for c in range(CHUNKS):
            sam_forward(from_relay, 1, c).wait_recv()

    loads[10].wait()

    def near_pair(m):
        base = (me - 1) * leaf_dev
        work = [(s, n) for s in range(2) for n in range(nn)]
        picked = [
            jnp.clip(near_ref[first_leaf + 2 * m + s, n] - base, 0, 3 * leaf_dev - 1) for s, n in work
        ]
        totals, dists = {}, {}
        for step in range(len(work) + LAG):
            if step < len(work):
                s, n = work[step]
                features = xfeat[n % 2, 2 * m + s]
                dists[step] = jnp.dot(yfeat[picked[step]], features, preferred_element_type=jnp.float32)
            if step >= LAG:
                s, n = work[step - LAG]
                block = lax.rsqrt(dists.pop(step - LAG).astype(jnp.bfloat16))
                values = wvec[picked[step - LAG]].reshape(both, leaf_pts)
                term = jnp.dot(values, block, preferred_element_type=jnp.float32)
                totals[s, n % 2] = term if n < 2 else totals[s, n % 2] + term
        for (s, lane), total in totals.items():
            near_all[lane, 2 * m + s] = total

    def pass_mate(step, carry):
        coef_across(step).wait_recv()
        mate_forward(step).start()
        return carry

    def fine_term(leaf, b):
        slot = farf_ref[first_leaf + leaf, b]
        source = lax.div(slot, cap0)
        index = source * leaf_dev + got_smem[source, 0, lax.rem(slot, cap0)]
        return nt(fine_all[index], cf_ref[leaf, b])

    def coarse_term(m, b):
        slot = farc_ref[first_parent + m, b]
        source = lax.div(slot, cap1)
        index = source * parents + got_smem[source, 1, lax.rem(slot, cap1)]
        return nt(coarse_all[index], cc_ref[m, b])

    def rows_copy(m, step):
        part = rows_all.at[g, :, :, pl.ds(pl.multiple_of(m * 2 * leaf_pts, 2 * leaf_pts), 2 * leaf_pts)]
        return remote(part, part, rows_send.at[step, m], rows_recv.at[step, m], group_peer(step))

    def out_copy(m):
        columns = pl.ds(pl.multiple_of(m * 2 * leaf_pts, 2 * leaf_pts), 2 * leaf_pts)
        start = (first_leaf + 2 * m) * leaf_pts
        there = pl.ds(pl.multiple_of(start, 2 * leaf_pts), 2 * leaf_pts)
        return remote(
            rows_all.at[g, 1 - h, :, columns], out_ref.at[:, there], out_send.at[m], out_recv.at[m], partner
        )

    def far_field():
        def finish(step, carry):
            table_copy(step).wait()
            return carry

        def arrive(step, carry):
            coef_forward(step).wait_recv()
            mate_forward(step).wait_recv()
            return carry

        lax.fori_loop(1, devices, finish, 0)
        lax.fori_loop(0, columns, arrive, 0)
        to_smem = pltpu.make_async_copy(got, got_smem, local_sem.at[13])
        to_smem.start()

        def unpack(d, carry):
            for m in range(parents):
                pair = coef_pk[d, m].reshape(both, 2 * basis_rank)
                fine_all[d * leaf_dev + 2 * m] = pair[:, :basis_rank]
                fine_all[d * leaf_dev + 2 * m + 1] = pair[:, basis_rank:]
            for m in range(half_parents):
                pair = coef_pk[d, parents + m].reshape(both, 2 * basis_rank)
                coarse_all[d * parents + 2 * m] = pair[:, :basis_rank]
                coarse_all[d * parents + 2 * m + 1] = pair[:, basis_rank:]
            return carry

        lax.fori_loop(0, devices, unpack, 0)
        for n in (8, 9, 11, 12):
            loads[n].wait()
        to_smem.wait()
        coarse_field = []
        for m in range(half_parents):
            field = coarse_term(m, 0)
            for b in range(1, nbc):
                field = field + coarse_term(m, b)
            coarse_field.append(field.astype(jnp.bfloat16))
        for leaf in range(half_leaves):
            field = nt(coarse_field[leaf // 2], transfer_ref[first_parent + leaf // 2, leaf % 2])
            for b in range(nb):
                field = field + fine_term(leaf, b)
            local_ref[leaf] = field.astype(jnp.bfloat16)

    def emit(m):
        for s in range(2):
            leaf = 2 * m + s
            far = jnp.dot(local_ref[leaf], basis_ref[first_leaf + leaf], preferred_element_type=jnp.float32)
            result = (near_all[0, leaf] + near_all[1, leaf] + far).astype(out_ref.dtype)
            result = result.reshape(2, vec_dev, leaf_pts)
            rows_all[g, :, :, cut(leaf)] = result
        for step in range(1, groups):
            rows_copy(m, step).start()
        out_copy(m).start()

    def near_step(m, carry):
        near_pair(m)

        @pl.when(m == MATE_AT)
        def _():
            lax.fori_loop(0, columns, pass_mate, 0)

        @pl.when(m == FAR_AT)
        def _():
            far_field()
            for done in range(FAR_AT):
                emit(done)

        @pl.when(m >= FAR_AT)
        def _():
            emit(m)
        return carry

    lax.fori_loop(0, half_parents, near_step, 0)

    for leaf in range(half_leaves):
        out_ref[:, cut(first_leaf + leaf)] = rows_all[g, h, :, cut(leaf)]

    def gram_pair(m, carry):
        for step in range(1, groups):
            rows_copy(m, step).wait()
        for s in range(2):
            leaf = 2 * m + s
            everyone = rows_all[:, :, :, cut(leaf)].reshape(vecs * vec_dev, leaf_pts)
            gram_ref[first_leaf + leaf] = nt(rows_all[g, h, :, cut(leaf)], everyone) * (1.0 / leaf_pts)
            gram_out[leaf] = nt(rows_all[g, 1 - h, :, cut(leaf)], everyone) * (1.0 / leaf_pts)
        return carry

    lax.fori_loop(0, half_parents, gram_pair, 0)
    gram_copy = remote(
        gram_out, gram_ref.at[pl.ds(first_leaf, half_leaves)], gram_send.at[0], gram_recv.at[0], partner
    )
    gram_copy.start()

    geo_copy().wait_send()
    geo_forward(from_mate, 0).wait_send()
    own_forward().wait_send()
    for c in range(CHUNKS):
        sam_copy(c).wait_send()
        sam_forward(from_mate, 0, c).wait_send()

    @pl.when(sends_on)
    def _():
        geo_relay().wait_send()
        for c in range(CHUNKS):
            sam_relay(c).wait_send()

    @pl.when(gets_relay)
    def _():
        geo_forward(from_relay, 1).wait_send()
        for c in range(CHUNKS):
            sam_forward(from_relay, 1, c).wait_send()

    def drain(step, carry):
        coef_across(step).wait_send()
        coef_forward(step).wait_send()
        mate_forward(step).wait_send()
        return carry

    def drain_copy(step, carry):
        coef_copy(step).wait_send()
        return carry

    lax.fori_loop(0, columns, drain, 0)
    lax.fori_loop(1, columns, drain_copy, 0)
    for m in range(half_parents):
        out_copy(m).wait()
    gram_copy.wait()


def per_device(
    samples, coords, panel_area, quad_weight, leaf_basis, transfer,
    coupling_fine, coupling_coarse, near_list, send_fine, send_coarse, far_fine, far_coarse,
):
    vec_dev, points = samples.shape
    leaf_dev, basis_rank, leaf_pts = leaf_basis.shape
    parents, half = leaf_dev // 2, leaf_dev // 2
    devices, vecs = lax.axis_size("leaf"), lax.axis_size("vec")
    groups, both = vecs // 2, 2 * vec_dev
    nb, nbc = coupling_fine.shape[1], coupling_coarse.shape[1]
    vmem = pl.BlockSpec(memory_space=pltpu.VMEM)
    hbm = pl.BlockSpec(memory_space=pl.ANY)
    bf16, f32 = jnp.bfloat16, jnp.float32
    dma = pltpu.SemaphoreType.DMA
    sample_out, gram = pl.pallas_call(
        main_kernel,
        out_shape=(
            jax.ShapeDtypeStruct((vec_dev, points), bf16),
            jax.ShapeDtypeStruct((leaf_dev, vec_dev, vecs * vec_dev), f32),
        ),
        in_specs=[hbm] * 13,
        out_specs=(vmem, vmem),
        scratch_shapes=[
            pltpu.SMEM(near_list.shape, jnp.int32),
            pltpu.SMEM(far_fine.shape, jnp.int32),
            pltpu.SMEM(far_coarse.shape, jnp.int32),
            pltpu.VMEM(coords.shape, f32),
            pltpu.VMEM((1, points), f32),
            pltpu.VMEM((1, points), f32),
            pltpu.VMEM(samples.shape, bf16),
            pltpu.VMEM(send_fine.shape, jnp.int32),
            pltpu.VMEM(send_coarse.shape, jnp.int32),
            pltpu.VMEM(transfer.shape, bf16),
            pltpu.VMEM(leaf_basis.shape, bf16),
            pltpu.VMEM((3 * leaf_dev, 4, leaf_pts), f32),
            pltpu.VMEM((3 * leaf_dev, 2, vec_dev, leaf_pts), bf16),
            pltpu.VMEM((devices, 2, 128), jnp.int32),
            pltpu.VMEM((devices, 2, 128), jnp.int32),
            pltpu.SMEM((devices, 2, 128), jnp.int32),
            pltpu.VMEM((devices, parents + parents // 2, 2, vec_dev, 2 * basis_rank), bf16),
            pltpu.VMEM((devices * leaf_dev, both, basis_rank), bf16),
            pltpu.VMEM((devices * parents, both, basis_rank), bf16),
            pltpu.VMEM((half, nb, basis_rank, basis_rank), bf16),
            pltpu.VMEM((half // 2, nbc, basis_rank, basis_rank), bf16),
            pltpu.VMEM((3 * leaf_dev, leaf_pts, 48), bf16),
            pltpu.VMEM((2, half, 48, leaf_pts), bf16),
            pltpu.VMEM((2, half, both, leaf_pts), f32),
            pltpu.VMEM((half, both, basis_rank), bf16),
            pltpu.VMEM((groups, 2, vec_dev, half * leaf_pts), bf16),
            pltpu.VMEM((half, vec_dev, vecs * vec_dev), f32),
            dma((2,)), dma((2,)), dma((2,)), dma((2,)),
            dma((2, CHUNKS)), dma((2, CHUNKS)), dma((2, CHUNKS)), dma((2, CHUNKS)), dma((1,)), dma((1,)),
            dma((devices,)), dma((devices,)),
            dma((devices // 2,)), dma((devices // 2,)), dma((devices // 2,)), dma((devices // 2,)),
            dma((2, devices // 2)), dma((2, devices // 2)),
            dma((groups, half // 2)), dma((groups, half // 2)),
            dma((half // 2,)), dma((half // 2,)),
            dma((1,)), dma((1,)),
            dma((14,)),
        ],
        compiler_params=pltpu.CompilerParams(
            vmem_limit_bytes=56 * 1024 * 1024, collective_id=0, has_side_effects=True
        ),
    )(
        near_list, far_fine, far_coarse,
        coords, panel_area[None, :], quad_weight[None, :], samples, send_fine, send_coarse,
        transfer, leaf_basis, coupling_fine, coupling_coarse,
    )
    return sample_out, gram


def solution(mesh):
    return jax.shard_map(
        per_device,
        mesh=mesh,
        in_specs=(
            P("vec", "leaf"), P(None, "leaf"), P("leaf"), P("leaf"),
            P("leaf", None, None), P("leaf", None, None, None),
            P("leaf", None, None, None), P("leaf", None, None, None),
            P("leaf", None), P("leaf", None), P("leaf", None), P("leaf", None), P("leaf", None),
        ),
        out_specs=(P("vec", "leaf"), P("leaf", "vec", None)),
        check_vma=False,
    )
```

```python
import functools
import jax
import jax.numpy as jnp
from jax import lax
from jax.experimental import pallas as pl
from jax.experimental.pallas import tpu as pltpu
from jax.sharding import PartitionSpec as P

four_pi = 4.0 * 3.141592653589793
NT = (((1,), (1,)), ((), ()))
MESH = pl.DeviceIdType.MESH
LAG = 4
CHUNKS = 4
DIRECT = 1
GEO_DIRECT = False
RELAYED = CHUNKS - DIRECT
MATE_AT, FAR_AT = 1, 2


def pieces(block):
    first = block.astype(jnp.bfloat16).astype(jnp.float32)
    rest = block - first
    second = rest.astype(jnp.bfloat16).astype(jnp.float32)
    return first, second, rest - second


def main_kernel(
    near_hbm, farf_hbm, farc_hbm,
    coords_hbm, area_hbm, weight_hbm, sam_hbm, sendf_hbm, sendc_hbm, transfer_hbm, basis_hbm, cf_hbm, cc_hbm,
    out_ref, gram_ref,
    near_ref, farf_ref, farc_ref,
    coords_ref, area_ref, weight_ref, sam_ref, sendf_ref, sendc_ref, transfer_ref, basis_ref,
    geo_all, wvec, table, got, got_smem, coef_pk, fine_all, coarse_all, cf_ref, cc_ref,
    yfeat, xfeat, near_all, local_ref, rows_all, gram_out,
    geo_send, geo_recv, geo_fsend, geo_frecv, sam_send, sam_recv, sam_fsend, sam_frecv, own_send, own_recv,
    table_send, table_recv, coef_send, coef_recv, mate_send, mate_recv, coef_fsend, coef_frecv,
    rows_send, rows_recv, out_send, out_recv, gram_send, gram_recv, local_sem,
):
    leaf_dev, basis_rank, leaf_pts = basis_ref.shape
    vec_dev = sam_ref.shape[0]
    parents = leaf_dev // 2
    cap0, cap1 = sendf_ref.shape[1], sendc_ref.shape[1]
    nb = farf_ref.shape[1]
    nbc = farc_ref.shape[1]
    nn = near_ref.shape[1]
    half_leaves, half_parents = leaf_dev // 2, parents // 2
    both = 2 * vec_dev
    chunk = leaf_dev // CHUNKS
    devices, vecs = lax.axis_size("leaf"), lax.axis_size("vec")
    groups, columns = vecs // 2, devices // 2
    me, row = lax.axis_index("leaf"), lax.axis_index("vec")
    h, g = lax.rem(row, 2), lax.div(row, 2)
    partner = {"vec": row + 1 - 2 * h}
    first_leaf, first_parent = h * half_leaves, h * half_parents

    def leaf_peer(step):
        return {"leaf": lax.rem(me + step, devices)}

    def group_peer(step):
        return {"vec": lax.rem(g + step, groups) * 2 + h}

    def remote(src, dst, send, recv, peer):
        return pltpu.make_async_remote_copy(
            src_ref=src, dst_ref=dst, send_sem=send, recv_sem=recv,
            device_id=peer, device_id_type=MESH,
        )

    def cut(leaf):
        return pl.ds(pl.multiple_of(leaf * leaf_pts, leaf_pts), leaf_pts)

    def nt(a, b):
        return lax.dot_general(a, b, NT, preferred_element_type=jnp.float32)

    loads = [
        pltpu.make_async_copy(src, dst, local_sem.at[n])
        for n, (src, dst) in enumerate([
            (coords_hbm, coords_ref), (area_hbm, area_ref), (weight_hbm, weight_ref), (sam_hbm, sam_ref),
            (sendf_hbm, sendf_ref), (sendc_hbm, sendc_ref), (basis_hbm, basis_ref), (transfer_hbm, transfer_ref),
            (cf_hbm.at[pl.ds(first_leaf, half_leaves)], cf_ref),
            (cc_hbm.at[pl.ds(first_parent, half_parents)], cc_ref),
            (near_hbm, near_ref), (farf_hbm, farf_ref), (farc_hbm, farc_ref),
        ])
    ]
    for load in loads:
        load.start()
    barrier = pltpu.get_barrier_semaphore()

    def greet(step, carry):
        pl.semaphore_signal(barrier, inc=1, device_id=leaf_peer(step), device_id_type=MESH)
        return carry

    lax.fori_loop(1, devices, greet, 0)
    pl.semaphore_signal(barrier, inc=1, device_id=partner, device_id_type=MESH)
    for step in range(1, groups):
        pl.semaphore_signal(barrier, inc=1, device_id=group_peer(step), device_id_type=MESH)

    for load in loads[:6]:
        load.wait()

    def own(leaf, carry):
        xyz = coords_ref[:, cut(leaf)]
        norm = jnp.sum(xyz * xyz, axis=0, keepdims=True) + area_ref[:, cut(leaf)]
        geo_all[leaf_dev + leaf] = jnp.concatenate([xyz, norm], axis=0)
        weight = weight_ref[:, cut(leaf)] * (1.0 / four_pi)
        scaled = sam_ref[:, cut(leaf)].astype(jnp.float32) * weight
        wvec[leaf_dev + leaf, h] = scaled.astype(jnp.bfloat16)
        return carry

    lax.fori_loop(0, leaf_dev, own, 0, unroll=4)
    table[...] = jnp.zeros_like(table)

    def fill(d, carry):
        table[d, 0:1, 0:cap0] = sendf_ref[pl.ds(d, 1), :]
        table[d, 1:2, 0:cap1] = sendc_ref[pl.ds(d, 1), :]
        return carry

    lax.fori_loop(0, devices, fill, 0)
    got[me] = table[me]
    pl.semaphore_wait(barrier, devices - 1 + 1 + groups - 1)

    odd = lax.rem(me, 2)
    mate = {"leaf": me + 1 - 2 * odd}
    from_mate, from_relay = 2 * (1 - odd), 2 * odd
    onward = {"leaf": me + 2 - 4 * odd}
    other = {"leaf": me - 1 + 2 * odd}
    sends_on = jnp.where(odd == 0, me + 2 < devices, me >= 2)
    gets_relay = jnp.where(odd == 0, me >= 2, me + 2 < devices)

    def geo_part(part):
        return geo_all.at[pl.ds(part * leaf_dev + first_leaf, half_leaves)]

    def sam_part(part, c):
        return wvec.at[pl.ds(part * leaf_dev + c * chunk, chunk), h]

    def geo_copy():
        return remote(geo_part(1), geo_part(from_relay), geo_send.at[0], geo_recv.at[0], mate)

    def geo_relay():
        if GEO_DIRECT:
            return remote(geo_part(1), geo_part(from_mate), geo_send.at[1], geo_recv.at[1], other)
        return remote(geo_part(from_mate), geo_part(from_relay), geo_send.at[1], geo_recv.at[1], onward)

    def geo_forward(part, n):
        return remote(geo_part(part), geo_part(part), geo_fsend.at[n], geo_frecv.at[n], partner)

    def sam_copy(c):
        return remote(sam_part(1, c), sam_part(from_relay, c), sam_send.at[0, c], sam_recv.at[0, c], mate)

    def sam_relay(c):
        return remote(sam_part(from_mate, c), sam_part(from_relay, c), sam_send.at[1, c], sam_recv.at[1, c], onward)

    def sam_direct(c):
        return remote(sam_part(1, c), sam_part(from_mate, c), sam_send.at[1, c], sam_recv.at[1, c], other)

    def sam_forward(part, n, c):
        block = sam_part(part, c)
        return remote(block, block, sam_fsend.at[n, c], sam_frecv.at[n, c], partner)

    def own_forward():
        block = wvec.at[pl.ds(leaf_dev, leaf_dev), h]
        return remote(block, block, own_send.at[0], own_recv.at[0], partner)

    def table_copy(step):
        peer = lax.rem(me + step, devices)
        return remote(table.at[peer], got.at[me], table_send.at[step], table_recv.at[step], {"leaf": peer})

    def same(step):
        return lax.rem(me + 2 * step, devices)

    def block_from(step):
        return lax.rem(me - 2 * step + devices, devices)

    def mate_block(step):
        return lax.rem(me + 1 - 2 * odd - 2 * step + devices, devices)

    def coef_copy(step):
        part = coef_pk.at[me, :, h]
        return remote(part, part, coef_send.at[step], coef_recv.at[step], {"leaf": same(step)})

    def coef_across(step):
        part = coef_pk.at[block_from(step), :, h]
        return remote(part, part, mate_send.at[step], mate_recv.at[step], mate)

    def coef_forward(step):
        part = coef_pk.at[block_from(step), :, h]
        return remote(part, part, coef_fsend.at[0, step], coef_frecv.at[0, step], partner)

    def mate_forward(step):
        part = coef_pk.at[mate_block(step), :, h]
        return remote(part, part, coef_fsend.at[1, step], coef_frecv.at[1, step], partner)

    geo_copy().start()
    if GEO_DIRECT:

        @pl.when(gets_relay)
        def _():
            geo_relay().start()

    sam_copy(0).start()

    @pl.when(gets_relay)
    def _():
        for c in range(RELAYED, CHUNKS):
            sam_direct(c).start()

    for c in range(1, CHUNKS):
        sam_copy(c).start()
    own_forward().start()

    def start_table(step, carry):
        table_copy(step).start()
        return carry

    lax.fori_loop(1, devices, start_table, 0)

    loads[6].wait()
    loads[7].wait()
    blank = jnp.zeros((basis_rank, leaf_pts), jnp.bfloat16)
    packed = []
    for m in range(parents):
        left = jnp.concatenate([basis_ref[2 * m], blank], axis=0)
        right = jnp.concatenate([blank, basis_ref[2 * m + 1]], axis=0)
        coef = nt(sam_ref[:, cut(2 * m)], left) + nt(sam_ref[:, cut(2 * m + 1)], right)
        coef = coef.astype(jnp.bfloat16)
        coef_pk[me, m, h] = coef
        packed.append(coef)
    coarse = []
    for m in range(parents):
        both_children = transfer_ref[m].reshape(2 * basis_rank, basis_rank)
        coarse.append(jnp.dot(packed[m], both_children, preferred_element_type=jnp.float32))
    for m in range(half_parents):
        pair = jnp.concatenate([coarse[2 * m], coarse[2 * m + 1]], axis=1)
        coef_pk[me, parents + m, h] = pair.astype(jnp.bfloat16)

    def start_coef(step, carry):
        coef_copy(step).start()
        return carry

    lax.fori_loop(1, columns, start_coef, 0)
    coef_across(0).start()
    coef_forward(0).start()

    def prepare(part):
        def source(leaf, carry):
            geo = geo_all[part * leaf_dev + leaf]
            ones = jnp.ones((1, leaf_pts), jnp.float32)
            rows = jnp.concatenate([geo, ones, jnp.zeros((3, leaf_pts), jnp.float32)], axis=0)
            y1, y2, y3 = pieces(rows)
            rows = jnp.concatenate([y1, y1, y1, y2, y2, y3], axis=0)
            yfeat[part * leaf_dev + leaf] = rows.T.astype(jnp.bfloat16)
            return carry

        lax.fori_loop(0, leaf_dev, source, 0, unroll=4)

    prepare(1)

    def target(leaf, carry):
        xyz = geo_all[leaf_dev + first_leaf + leaf][0:3]
        norm = jnp.sum(xyz * xyz, axis=0, keepdims=True)
        x8 = jnp.concatenate(
            [-2.0 * xyz, jnp.ones_like(norm), norm, jnp.zeros_like(xyz)], axis=0
        )
        x1, x2, x3 = pieces(x8)
        features = jnp.concatenate([x1, x2, x3, x1, x2, x1], axis=0).astype(jnp.bfloat16)
        xfeat[0, leaf] = features
        xfeat[1, leaf] = features
        return carry

    lax.fori_loop(0, half_leaves, target, 0, unroll=2)

    def pass_coef(step, carry):
        coef_copy(step).wait_recv()
        coef_across(step).start()
        coef_forward(step).start()
        return carry

    def pass_mate_sam(c):
        sam_copy(c).wait_recv()

        if c < RELAYED:

            @pl.when(sends_on)
            def _():
                sam_relay(c).start()

        sam_forward(from_mate, 0, c).start()

    geo_copy().wait_recv()

    if not GEO_DIRECT:

        @pl.when(sends_on)
        def _():
            geo_relay().start()

    geo_forward(from_mate, 0).start()
    pass_mate_sam(0)
    geo_forward(from_mate, 0).wait_recv()
    prepare(from_mate)
    for c in range(1, CHUNKS):
        pass_mate_sam(c)
    lax.fori_loop(1, columns, pass_coef, 0)

    @pl.when(gets_relay)
    def _():
        geo_relay().wait_recv()
        geo_forward(from_relay, 1).start()
        geo_forward(from_relay, 1).wait_recv()
        prepare(from_relay)
        for c in range(CHUNKS):
            sam_relay(c).wait_recv()
            sam_forward(from_relay, 1, c).start()

    own_forward().wait_recv()
    for c in range(CHUNKS):
        sam_forward(from_mate, 0, c).wait_recv()

    @pl.when(gets_relay)
    def _():
        for c in range(CHUNKS):
            sam_forward(from_relay, 1, c).wait_recv()

    loads[10].wait()

    def near_pair(m):
        base = (me - 1) * leaf_dev
        work = [(s, n) for s in range(2) for n in range(nn)]
        picked = [
            jnp.clip(near_ref[first_leaf + 2 * m + s, n] - base, 0, 3 * leaf_dev - 1) for s, n in work
        ]
        totals, dists = {}, {}
        for step in range(len(work) + LAG):
            if step < len(work):
                s, n = work[step]
                features = xfeat[n % 2, 2 * m + s]
                dists[step] = jnp.dot(yfeat[picked[step]], features, preferred_element_type=jnp.float32)
            if step >= LAG:
                s, n = work[step - LAG]
                block = lax.rsqrt(dists.pop(step - LAG).astype(jnp.bfloat16))
                values = wvec[picked[step - LAG]].reshape(both, leaf_pts)
                term = jnp.dot(values, block, preferred_element_type=jnp.float32)
                totals[s, n % 2] = term if n < 2 else totals[s, n % 2] + term
        for (s, lane), total in totals.items():
            near_all[lane, 2 * m + s] = total

    def pass_mate(step, carry):
        coef_across(step).wait_recv()
        mate_forward(step).start()
        return carry

    def fine_term(leaf, b):
        slot = farf_ref[first_leaf + leaf, b]
        source = lax.div(slot, cap0)
        index = source * leaf_dev + got_smem[source, 0, lax.rem(slot, cap0)]
        return nt(fine_all[index], cf_ref[leaf, b])

    def coarse_term(m, b):
        slot = farc_ref[first_parent + m, b]
        source = lax.div(slot, cap1)
        index = source * parents + got_smem[source, 1, lax.rem(slot, cap1)]
        return nt(coarse_all[index], cc_ref[m, b])

    def rows_copy(m, step):
        part = rows_all.at[g, :, :, pl.ds(pl.multiple_of(m * 2 * leaf_pts, 2 * leaf_pts), 2 * leaf_pts)]
        return remote(part, part, rows_send.at[step, m], rows_recv.at[step, m], group_peer(step))

    def out_copy(m):
        columns = pl.ds(pl.multiple_of(m * 2 * leaf_pts, 2 * leaf_pts), 2 * leaf_pts)
        start = (first_leaf + 2 * m) * leaf_pts
        there = pl.ds(pl.multiple_of(start, 2 * leaf_pts), 2 * leaf_pts)
        return remote(
            rows_all.at[g, 1 - h, :, columns], out_ref.at[:, there], out_send.at[m], out_recv.at[m], partner
        )

    def far_field():
        def finish(step, carry):
            table_copy(step).wait()
            return carry

        def arrive(step, carry):
            coef_forward(step).wait_recv()
            mate_forward(step).wait_recv()
            return carry

        lax.fori_loop(1, devices, finish, 0)
        lax.fori_loop(0, columns, arrive, 0)
        to_smem = pltpu.make_async_copy(got, got_smem, local_sem.at[13])
        to_smem.start()

        def unpack(d, carry):
            for m in range(parents):
                pair = coef_pk[d, m].reshape(both, 2 * basis_rank)
                fine_all[d * leaf_dev + 2 * m] = pair[:, :basis_rank]
                fine_all[d * leaf_dev + 2 * m + 1] = pair[:, basis_rank:]
            for m in range(half_parents):
                pair = coef_pk[d, parents + m].reshape(both, 2 * basis_rank)
                coarse_all[d * parents + 2 * m] = pair[:, :basis_rank]
                coarse_all[d * parents + 2 * m + 1] = pair[:, basis_rank:]
            return carry

        lax.fori_loop(0, devices, unpack, 0, unroll=4)
        for n in (8, 9, 11, 12):
            loads[n].wait()
        to_smem.wait()
        coarse_field = []
        for m in range(half_parents):
            field = coarse_term(m, 0)
            for b in range(1, nbc):
                field = field + coarse_term(m, b)
            coarse_field.append(field.astype(jnp.bfloat16))
        for leaf in range(half_leaves):
            field = fine_term(leaf, 0)
            for b in range(1, nb):
                field = field + fine_term(leaf, b)
            field = field + nt(coarse_field[leaf // 2], transfer_ref[first_parent + leaf // 2, leaf % 2])
            local_ref[leaf] = field.astype(jnp.bfloat16)

    def emit(m):
        for s in range(2):
            leaf = 2 * m + s
            far = jnp.dot(local_ref[leaf], basis_ref[first_leaf + leaf], preferred_element_type=jnp.float32)
            result = (near_all[0, leaf] + near_all[1, leaf] + far).astype(out_ref.dtype)
            result = result.reshape(2, vec_dev, leaf_pts)
            rows_all[g, :, :, cut(leaf)] = result
        for step in range(1, groups):
            rows_copy(m, step).start()
        out_copy(m).start()

    def near_step(m, carry):
        near_pair(m)

        @pl.when(m == MATE_AT)
        def _():
            lax.fori_loop(0, columns, pass_mate, 0)

        @pl.when(m == FAR_AT)
        def _():
            far_field()
            for done in range(FAR_AT):
                emit(done)

        @pl.when(m >= FAR_AT)
        def _():
            emit(m)
        return carry

    lax.fori_loop(0, half_parents, near_step, 0)

    for leaf in range(half_leaves):
        out_ref[:, cut(first_leaf + leaf)] = rows_all[g, h, :, cut(leaf)]

    def gram_pair(m, carry):
        for step in range(1, groups):
            rows_copy(m, step).wait()
        for s in range(2):
            leaf = 2 * m + s
            everyone = rows_all[:, :, :, cut(leaf)].reshape(vecs * vec_dev, leaf_pts)
            gram_ref[first_leaf + leaf] = nt(rows_all[g, h, :, cut(leaf)], everyone) * (1.0 / leaf_pts)
            gram_out[leaf] = nt(rows_all[g, 1 - h, :, cut(leaf)], everyone) * (1.0 / leaf_pts)
        return carry

    lax.fori_loop(0, half_parents, gram_pair, 0)
    gram_copy = remote(
        gram_out, gram_ref.at[pl.ds(first_leaf, half_leaves)], gram_send.at[0], gram_recv.at[0], partner
    )
    gram_copy.start()

    geo_copy().wait_send()
    geo_forward(from_mate, 0).wait_send()
    own_forward().wait_send()
    for c in range(CHUNKS):
        sam_copy(c).wait_send()
        sam_forward(from_mate, 0, c).wait_send()

    @pl.when(gets_relay if GEO_DIRECT else sends_on)
    def _():
        geo_relay().wait_send()

    @pl.when(sends_on)
    def _():
        for c in range(RELAYED):
            sam_relay(c).wait_send()

    @pl.when(gets_relay)
    def _():
        for c in range(RELAYED, CHUNKS):
            sam_direct(c).wait_send()
        geo_forward(from_relay, 1).wait_send()
        for c in range(CHUNKS):
            sam_forward(from_relay, 1, c).wait_send()

    def drain(step, carry):
        coef_across(step).wait_send()
        coef_forward(step).wait_send()
        mate_forward(step).wait_send()
        return carry

    def drain_copy(step, carry):
        coef_copy(step).wait_send()
        return carry

    lax.fori_loop(0, columns, drain, 0)
    lax.fori_loop(1, columns, drain_copy, 0)
    for m in range(half_parents):
        out_copy(m).wait()
    gram_copy.wait()


def write_kernel(out_ref, gram_ref, out_hbm, gram_hbm, sem):
    copies = [
        pltpu.make_async_copy(out_ref, out_hbm, sem.at[0]),
        pltpu.make_async_copy(gram_ref, gram_hbm, sem.at[1]),
    ]
    for copy in copies:
        copy.start()
    for copy in copies:
        copy.wait()


def per_device(
    samples, coords, panel_area, quad_weight, leaf_basis, transfer,
    coupling_fine, coupling_coarse, near_list, send_fine, send_coarse, far_fine, far_coarse,
):
    vec_dev, points = samples.shape
    leaf_dev, basis_rank, leaf_pts = leaf_basis.shape
    parents, half = leaf_dev // 2, leaf_dev // 2
    devices, vecs = lax.axis_size("leaf"), lax.axis_size("vec")
    groups, both = vecs // 2, 2 * vec_dev
    nb, nbc = coupling_fine.shape[1], coupling_coarse.shape[1]
    vmem = pl.BlockSpec(memory_space=pltpu.VMEM)
    hbm = pl.BlockSpec(memory_space=pl.ANY)
    bf16, f32 = jnp.bfloat16, jnp.float32
    dma = pltpu.SemaphoreType.DMA
    sample_out, gram = pl.pallas_call(
        main_kernel,
        out_shape=(
            pltpu.VMEM((vec_dev, points), bf16),
            pltpu.VMEM((leaf_dev, vec_dev, vecs * vec_dev), f32),
        ),
        in_specs=[hbm] * 13,
        out_specs=(vmem, vmem),
        scratch_shapes=[
            pltpu.SMEM(near_list.shape, jnp.int32),
            pltpu.SMEM(far_fine.shape, jnp.int32),
            pltpu.SMEM(far_coarse.shape, jnp.int32),
            pltpu.VMEM(coords.shape, f32),
            pltpu.VMEM((1, points), f32),
            pltpu.VMEM((1, points), f32),
            pltpu.VMEM(samples.shape, bf16),
            pltpu.VMEM(send_fine.shape, jnp.int32),
            pltpu.VMEM(send_coarse.shape, jnp.int32),
            pltpu.VMEM(transfer.shape, bf16),
            pltpu.VMEM(leaf_basis.shape, bf16),
            pltpu.VMEM((3 * leaf_dev, 4, leaf_pts), f32),
            pltpu.VMEM((3 * leaf_dev, 2, vec_dev, leaf_pts), bf16),
            pltpu.VMEM((devices, 2, 128), jnp.int32),
            pltpu.VMEM((devices, 2, 128), jnp.int32),
            pltpu.SMEM((devices, 2, 128), jnp.int32),
            pltpu.VMEM((devices, parents + parents // 2, 2, vec_dev, 2 * basis_rank), bf16),
            pltpu.VMEM((devices * leaf_dev, both, basis_rank), bf16),
            pltpu.VMEM((devices * parents, both, basis_rank), bf16),
            pltpu.VMEM((half, nb, basis_rank, basis_rank), bf16),
            pltpu.VMEM((half // 2, nbc, basis_rank, basis_rank), bf16),
            pltpu.VMEM((3 * leaf_dev, leaf_pts, 48), bf16),
            pltpu.VMEM((2, half, 48, leaf_pts), bf16),
            pltpu.VMEM((2, half, both, leaf_pts), f32),
            pltpu.VMEM((half, both, basis_rank), bf16),
            pltpu.VMEM((groups, 2, vec_dev, half * leaf_pts), bf16),
            pltpu.VMEM((half, vec_dev, vecs * vec_dev), f32),
            dma((2,)), dma((2,)), dma((2,)), dma((2,)),
            dma((2, CHUNKS)), dma((2, CHUNKS)), dma((2, CHUNKS)), dma((2, CHUNKS)), dma((1,)), dma((1,)),
            dma((devices,)), dma((devices,)),
            dma((devices // 2,)), dma((devices // 2,)), dma((devices // 2,)), dma((devices // 2,)),
            dma((2, devices // 2)), dma((2, devices // 2)),
            dma((groups, half // 2)), dma((groups, half // 2)),
            dma((half // 2,)), dma((half // 2,)),
            dma((1,)), dma((1,)),
            dma((14,)),
        ],
        compiler_params=pltpu.CompilerParams(
            vmem_limit_bytes=56 * 1024 * 1024, collective_id=0, has_side_effects=True
        ),
    )(
        near_list, far_fine, far_coarse,
        coords, panel_area[None, :], quad_weight[None, :], samples, send_fine, send_coarse,
        transfer, leaf_basis, coupling_fine, coupling_coarse,
    )
    return pl.pallas_call(
        write_kernel,
        out_shape=(
            jax.ShapeDtypeStruct(sample_out.shape, bf16),
            jax.ShapeDtypeStruct(gram.shape, f32),
        ),
        in_specs=[vmem] * 2,
        out_specs=(hbm, hbm),
        scratch_shapes=[dma((2,))],
    )(pltpu.with_memory_space_constraint(sample_out, pltpu.VMEM), pltpu.with_memory_space_constraint(gram, pltpu.VMEM))


def solution(mesh):
    return jax.shard_map(
        per_device,
        mesh=mesh,
        in_specs=(
            P("vec", "leaf"), P(None, "leaf"), P("leaf"), P("leaf"),
            P("leaf", None, None), P("leaf", None, None, None),
            P("leaf", None, None, None), P("leaf", None, None, None),
            P("leaf", None), P("leaf", None), P("leaf", None), P("leaf", None), P("leaf", None),
        ),
        out_specs=(P("vec", "leaf"), P("leaf", "vec", None)),
        check_vma=False,
    )
```

```python
import functools
import jax
import jax.numpy as jnp
from jax import lax
from jax.experimental import pallas as pl
from jax.experimental.pallas import tpu as pltpu
from jax.sharding import PartitionSpec as P

four_pi = 4.0 * 3.141592653589793
NT = (((1,), (1,)), ((), ()))
MESH = pl.DeviceIdType.MESH
LAG = 6
CHUNKS = 4
DIRECT = 1
GEO_DIRECT = False
RELAYED = CHUNKS - DIRECT
MATE_AT, FAR_AT = 1, 2


def pieces(block):
    first = block.astype(jnp.bfloat16).astype(jnp.float32)
    rest = block - first
    second = rest.astype(jnp.bfloat16).astype(jnp.float32)
    return first, second, rest - second


def main_kernel(
    near_hbm, farf_hbm, farc_hbm,
    coords_hbm, area_hbm, weight_hbm, sam_hbm, sendf_hbm, sendc_hbm, transfer_hbm, basis_hbm, cf_hbm, cc_hbm,
    out_ref, gram_ref,
    near_ref, farf_ref, farc_ref,
    coords_ref, area_ref, weight_ref, sam_ref, sendf_ref, sendc_ref, transfer_ref, basis_ref,
    geo_all, wvec, table, got, got_smem, coef_pk, fine_tab, coarse_tab, cf_ref, cc_ref, cf_pair, cc_pair,
    yfeat, xfeat, near_all, local_ref, rows_all, gram_out,
    geo_send, geo_recv, geo_fsend, geo_frecv, sam_send, sam_recv, sam_fsend, sam_frecv, own_send, own_recv,
    table_send, table_recv, coef_send, coef_recv, mate_send, mate_recv, coef_fsend, coef_frecv,
    rows_send, rows_recv, out_send, out_recv, gram_send, gram_recv, local_sem,
):
    leaf_dev, basis_rank, leaf_pts = basis_ref.shape
    vec_dev = sam_ref.shape[0]
    parents = leaf_dev // 2
    cap0, cap1 = sendf_ref.shape[1], sendc_ref.shape[1]
    nb = farf_ref.shape[1]
    nbc = farc_ref.shape[1]
    nn = near_ref.shape[1]
    half_leaves, half_parents = leaf_dev // 2, parents // 2
    both = 2 * vec_dev
    chunk = leaf_dev // CHUNKS
    devices, vecs = lax.axis_size("leaf"), lax.axis_size("vec")
    groups, columns = vecs // 2, devices // 2
    me, row = lax.axis_index("leaf"), lax.axis_index("vec")
    h, g = lax.rem(row, 2), lax.div(row, 2)
    partner = {"vec": row + 1 - 2 * h}
    first_leaf, first_parent = h * half_leaves, h * half_parents

    def leaf_peer(step):
        return {"leaf": lax.rem(me + step, devices)}

    def group_peer(step):
        return {"vec": lax.rem(g + step, groups) * 2 + h}

    def remote(src, dst, send, recv, peer):
        return pltpu.make_async_remote_copy(
            src_ref=src, dst_ref=dst, send_sem=send, recv_sem=recv,
            device_id=peer, device_id_type=MESH,
        )

    def cut(leaf):
        return pl.ds(pl.multiple_of(leaf * leaf_pts, leaf_pts), leaf_pts)

    def nt(a, b):
        return lax.dot_general(a, b, NT, preferred_element_type=jnp.float32)

    loads = [
        pltpu.make_async_copy(src, dst, local_sem.at[n])
        for n, (src, dst) in enumerate([
            (coords_hbm, coords_ref), (area_hbm, area_ref), (weight_hbm, weight_ref), (sam_hbm, sam_ref),
            (sendf_hbm, sendf_ref), (sendc_hbm, sendc_ref), (basis_hbm, basis_ref), (transfer_hbm, transfer_ref),
            (cf_hbm.at[pl.ds(first_leaf, half_leaves)], cf_ref),
            (cc_hbm.at[pl.ds(first_parent, half_parents)], cc_ref),
            (near_hbm, near_ref), (farf_hbm, farf_ref), (farc_hbm, farc_ref),
        ])
    ]
    for load in loads:
        load.start()
    barrier = pltpu.get_barrier_semaphore()

    def greet(step, carry):
        pl.semaphore_signal(barrier, inc=1, device_id=leaf_peer(step), device_id_type=MESH)
        return carry

    lax.fori_loop(1, devices, greet, 0)
    pl.semaphore_signal(barrier, inc=1, device_id=partner, device_id_type=MESH)
    for step in range(1, groups):
        pl.semaphore_signal(barrier, inc=1, device_id=group_peer(step), device_id_type=MESH)

    for load in loads[:6]:
        load.wait()

    def own(leaf, carry):
        xyz = coords_ref[:, cut(leaf)]
        norm = jnp.sum(xyz * xyz, axis=0, keepdims=True) + area_ref[:, cut(leaf)]
        geo_all[leaf_dev + leaf] = jnp.concatenate([xyz, norm], axis=0)
        weight = weight_ref[:, cut(leaf)] * (1.0 / four_pi)
        scaled = sam_ref[:, cut(leaf)].astype(jnp.float32) * weight
        wvec[leaf_dev + leaf, h] = scaled.astype(jnp.bfloat16)
        return carry

    lax.fori_loop(0, leaf_dev, own, 0, unroll=4)
    table[...] = jnp.zeros_like(table)

    def fill(d, carry):
        table[d, 0:1, 0:cap0] = sendf_ref[pl.ds(d, 1), :]
        table[d, 1:2, 0:cap1] = sendc_ref[pl.ds(d, 1), :]
        return carry

    lax.fori_loop(0, devices, fill, 0)
    got[me] = table[me]
    pl.semaphore_wait(barrier, devices - 1 + 1 + groups - 1)

    odd = lax.rem(me, 2)
    mate = {"leaf": me + 1 - 2 * odd}
    from_mate, from_relay = 2 * (1 - odd), 2 * odd
    onward = {"leaf": me + 2 - 4 * odd}
    other = {"leaf": me - 1 + 2 * odd}
    sends_on = jnp.where(odd == 0, me + 2 < devices, me >= 2)
    gets_relay = jnp.where(odd == 0, me >= 2, me + 2 < devices)

    def geo_part(part):
        return geo_all.at[pl.ds(part * leaf_dev + first_leaf, half_leaves)]

    def sam_part(part, c):
        return wvec.at[pl.ds(part * leaf_dev + c * chunk, chunk), h]

    def geo_copy():
        return remote(geo_part(1), geo_part(from_relay), geo_send.at[0], geo_recv.at[0], mate)

    def geo_relay():
        if GEO_DIRECT:
            return remote(geo_part(1), geo_part(from_mate), geo_send.at[1], geo_recv.at[1], other)
        return remote(geo_part(from_mate), geo_part(from_relay), geo_send.at[1], geo_recv.at[1], onward)

    def geo_forward(part, n):
        return remote(geo_part(part), geo_part(part), geo_fsend.at[n], geo_frecv.at[n], partner)

    def sam_copy(c):
        return remote(sam_part(1, c), sam_part(from_relay, c), sam_send.at[0], sam_recv.at[0, c], mate)

    def sam_relay(c):
        return remote(sam_part(from_mate, c), sam_part(from_relay, c), sam_send.at[1], sam_recv.at[1, c], onward)

    def sam_direct(c):
        return remote(sam_part(1, c), sam_part(from_mate, c), sam_send.at[2], sam_recv.at[1, c], other)

    def sam_forward(part, n, c):
        block = sam_part(part, c)
        return remote(block, block, sam_fsend.at[n], sam_frecv.at[n], partner)

    def settle(ref, send, recv):
        return remote(ref, ref, send, recv, partner)

    def chunks(part, count):
        return wvec.at[pl.ds(part * leaf_dev, count * chunk), h]

    def own_forward():
        block = wvec.at[pl.ds(leaf_dev, leaf_dev), h]
        return remote(block, block, own_send.at[0], own_recv.at[0], partner)

    def table_copy(step):
        peer = lax.rem(me + step, devices)
        return remote(table.at[peer], got.at[me], table_send.at[0], table_recv.at[0], {"leaf": peer})

    def same(step):
        return lax.rem(me + 2 * step, devices)

    def block_from(step):
        return lax.rem(me - 2 * step + devices, devices)

    def mate_block(step):
        return lax.rem(me + 1 - 2 * odd - 2 * step + devices, devices)

    def coef_copy(step):
        part = coef_pk.at[me, :, h]
        return remote(part, part, coef_send.at[0], coef_recv.at[step], {"leaf": same(step)})

    def coef_across(step):
        part = coef_pk.at[block_from(step), :, h]
        return remote(part, part, mate_send.at[0], mate_recv.at[step], mate)

    def coef_forward(step):
        part = coef_pk.at[block_from(step), :, h]
        return remote(part, part, coef_fsend.at[0], coef_frecv.at[0], partner)

    def mate_forward(step):
        part = coef_pk.at[mate_block(step), :, h]
        return remote(part, part, coef_fsend.at[0], coef_frecv.at[0], partner)

    geo_copy().start()
    if GEO_DIRECT:

        @pl.when(gets_relay)
        def _():
            geo_relay().start()

    sam_copy(0).start()

    @pl.when(gets_relay)
    def _():
        for c in range(RELAYED, CHUNKS):
            sam_direct(c).start()

    for c in range(1, CHUNKS):
        sam_copy(c).start()
    own_forward().start()

    def start_table(step, carry):
        table_copy(step).start()
        return carry

    lax.fori_loop(1, devices, start_table, 0)

    loads[6].wait()
    loads[7].wait()
    blank = jnp.zeros((basis_rank, leaf_pts), jnp.bfloat16)
    packed = []
    for m in range(parents):
        left = jnp.concatenate([basis_ref[2 * m], blank], axis=0)
        right = jnp.concatenate([blank, basis_ref[2 * m + 1]], axis=0)
        coef = nt(sam_ref[:, cut(2 * m)], left) + nt(sam_ref[:, cut(2 * m + 1)], right)
        coef = coef.astype(jnp.bfloat16)
        coef_pk[me, m, h] = coef
        packed.append(coef)
    coarse = []
    for m in range(parents):
        both_children = transfer_ref[m].reshape(2 * basis_rank, basis_rank)
        coarse.append(jnp.dot(packed[m], both_children, preferred_element_type=jnp.float32))
    for m in range(half_parents):
        pair = jnp.concatenate([coarse[2 * m], coarse[2 * m + 1]], axis=1)
        coef_pk[me, parents + m, h] = pair.astype(jnp.bfloat16)

    def start_coef(step, carry):
        coef_copy(step).start()
        return carry

    lax.fori_loop(1, columns, start_coef, 0)
    coef_across(0).start()
    coef_forward(0).start()

    def prepare(part):
        def source(leaf, carry):
            geo = geo_all[part * leaf_dev + leaf]
            ones = jnp.ones((1, leaf_pts), jnp.float32)
            rows = jnp.concatenate([geo, ones, jnp.zeros((3, leaf_pts), jnp.float32)], axis=0)
            y1, y2, y3 = pieces(rows)
            rows = jnp.concatenate([y1, y1, y1, y2, y2, y3], axis=0)
            yfeat[part * leaf_dev + leaf] = rows.T.astype(jnp.bfloat16)
            return carry

        lax.fori_loop(0, leaf_dev, source, 0, unroll=4)

    prepare(1)

    def target(leaf, carry):
        xyz = geo_all[leaf_dev + first_leaf + leaf][0:3]
        norm = jnp.sum(xyz * xyz, axis=0, keepdims=True)
        x8 = jnp.concatenate(
            [-2.0 * xyz, jnp.ones_like(norm), norm, jnp.zeros_like(xyz)], axis=0
        )
        x1, x2, x3 = pieces(x8)
        features = jnp.concatenate([x1, x2, x3, x1, x2, x1], axis=0).astype(jnp.bfloat16)
        xfeat[0, leaf] = features
        xfeat[1, leaf] = features
        return carry

    lax.fori_loop(0, half_leaves, target, 0, unroll=2)

    def pass_coef(step, carry):
        coef_copy(step).wait_recv()
        coef_across(step).start()
        coef_forward(step).start()
        return carry

    def pass_mate_sam(c):
        sam_copy(c).wait_recv()

        if c < RELAYED:

            @pl.when(sends_on)
            def _():
                sam_relay(c).start()

        sam_forward(from_mate, 0, c).start()

    geo_copy().wait_recv()

    if not GEO_DIRECT:

        @pl.when(sends_on)
        def _():
            geo_relay().start()

    geo_forward(from_mate, 0).start()
    pass_mate_sam(0)
    geo_forward(from_mate, 0).wait_recv()
    prepare(from_mate)
    for c in range(1, CHUNKS):
        pass_mate_sam(c)
    lax.fori_loop(1, columns, pass_coef, 0)

    loads[8].wait()
    loads[9].wait()

    def pair_up(src, dst):
        def one(i, carry):
            for b in range(src.shape[1] // 2):
                dst[i, b] = jnp.concatenate([src[i, 2 * b], src[i, 2 * b + 1]], axis=1)
            return carry

        lax.fori_loop(0, src.shape[0], one, 0, unroll=2)

    @pl.when(gets_relay)
    def _():
        geo_relay().wait_recv()
        geo_forward(from_relay, 1).start()

    pair_up(cf_ref, cf_pair)
    pair_up(cc_ref, cc_pair)

    @pl.when(gets_relay)
    def _():
        geo_forward(from_relay, 1).wait_recv()
        prepare(from_relay)
        for c in range(CHUNKS):
            sam_relay(c).wait_recv()
            sam_forward(from_relay, 1, c).start()

    own_forward().wait_recv()
    settle(chunks(from_mate, CHUNKS), sam_fsend.at[0], sam_frecv.at[0]).wait_recv()

    @pl.when(gets_relay)
    def _():
        settle(chunks(from_relay, CHUNKS), sam_fsend.at[1], sam_frecv.at[1]).wait_recv()

    loads[10].wait()

    def near_pair(m):
        base = (me - 1) * leaf_dev
        work = [(s, n) for s in range(2) for n in range(nn)]
        picked = [
            jnp.clip(near_ref[first_leaf + 2 * m + s, n] - base, 0, 3 * leaf_dev - 1) for s, n in work
        ]
        totals, dists = {}, {}
        for step in range(len(work) + LAG):
            if step < len(work):
                s, n = work[step]
                features = xfeat[n % 2, 2 * m + s]
                dists[step] = jnp.dot(yfeat[picked[step]], features, preferred_element_type=jnp.float32)
            if step >= LAG:
                s, n = work[step - LAG]
                block = lax.rsqrt(dists.pop(step - LAG).astype(jnp.bfloat16))
                values = wvec[picked[step - LAG]].reshape(both, leaf_pts)
                term = jnp.dot(values, block, preferred_element_type=jnp.float32)
                totals[s, n % 2] = term if n < 2 else totals[s, n % 2] + term
        for (s, lane), total in totals.items():
            near_all[lane, 2 * m + s] = total

    def pass_mate(step, carry):
        coef_across(step).wait_recv()
        mate_forward(step).start()
        return carry

    left_lanes = lax.broadcasted_iota(jnp.int32, (both, 2 * basis_rank), 1) < basis_rank

    def split(slot, cap):
        if cap & (cap - 1):
            return lax.div(slot, cap), lax.rem(slot, cap)
        return slot >> (cap.bit_length() - 1), slot & (cap - 1)

    def pair_term(tab, tiles, far_ref, at, cap, line, per_device, b):
        rows = []
        for lane in range(2):
            slot = far_ref[at, 2 * b + lane]
            source, place = split(slot, cap)
            index = source * per_device + got_smem[source, line, place]
            rows.append(tab[index ^ lane])
        return nt(jnp.where(left_lanes, rows[0], rows[1]), tiles[b])

    def fine_term(leaf, b):
        return pair_term(fine_tab, cf_pair.at[leaf], farf_ref, first_leaf + leaf, cap0, 0, leaf_dev, b)

    def coarse_term(m, b):
        return pair_term(coarse_tab, cc_pair.at[m], farc_ref, first_parent + m, cap1, 1, parents, b)

    def rows_copy(m, step):
        part = rows_all.at[g, :, :, pl.ds(pl.multiple_of(m * 2 * leaf_pts, 2 * leaf_pts), 2 * leaf_pts)]
        return remote(part, part, rows_send.at[step - 1], rows_recv.at[step - 1, m], group_peer(step))

    def out_copy(m):
        columns = pl.ds(pl.multiple_of(m * 2 * leaf_pts, 2 * leaf_pts), 2 * leaf_pts)
        start = (first_leaf + 2 * m) * leaf_pts
        there = pl.ds(pl.multiple_of(start, 2 * leaf_pts), 2 * leaf_pts)
        return remote(
            rows_all.at[g, 1 - h, :, columns], out_ref.at[:, there], out_send.at[0], out_recv.at[0], partner
        )

    def far_field():
        settle(got.at[pl.ds(0, devices - 1)], table_send.at[0], table_recv.at[0]).wait()
        settle(coef_pk.at[:, :, 1 - h], coef_fsend.at[0], coef_frecv.at[0]).wait_recv()
        to_smem = pltpu.make_async_copy(got, got_smem, local_sem.at[13])
        to_smem.start()

        def unpack(d, carry):
            for tab, count, first in ((fine_tab, parents, 0), (coarse_tab, half_parents, parents)):
                for m in range(count):
                    pair = coef_pk[d, first + m].reshape(both, 2 * basis_rank)
                    tab[2 * (d * count + m)] = pair
                    tab[2 * (d * count + m) + 1] = jnp.concatenate(
                        [pair[:, basis_rank:], pair[:, :basis_rank]], axis=1
                    )
            return carry

        lax.fori_loop(0, devices, unpack, 0, unroll=4)
        loads[11].wait()
        loads[12].wait()
        to_smem.wait()
        coarse_field = []
        for m in range(half_parents):
            field = coarse_term(m, 0)
            for b in range(1, nbc // 2):
                field = field + coarse_term(m, b)
            coarse_field.append(field.astype(jnp.bfloat16))
        for leaf in range(half_leaves):
            field = fine_term(leaf, 0)
            for b in range(1, nb // 2):
                field = field + fine_term(leaf, b)
            field = field + nt(coarse_field[leaf // 2], transfer_ref[first_parent + leaf // 2, leaf % 2])
            local_ref[leaf] = field.astype(jnp.bfloat16)

    def emit(m):
        for s in range(2):
            leaf = 2 * m + s
            far = jnp.dot(local_ref[leaf], basis_ref[first_leaf + leaf], preferred_element_type=jnp.float32)
            result = (near_all[0, leaf] + near_all[1, leaf] + far).astype(out_ref.dtype)
            result = result.reshape(2, vec_dev, leaf_pts)
            rows_all[g, :, :, cut(leaf)] = result
        for step in range(1, groups):
            rows_copy(m, step).start()
        out_copy(m).start()

    def near_step(m, carry):
        near_pair(m)

        @pl.when(m == MATE_AT)
        def _():
            lax.fori_loop(0, columns, pass_mate, 0)

        @pl.when(m == FAR_AT)
        def _():
            far_field()
            for done in range(FAR_AT):
                emit(done)

        @pl.when(m >= FAR_AT)
        def _():
            emit(m)
        return carry

    lax.fori_loop(0, half_parents, near_step, 0)

    for leaf in range(half_leaves):
        out_ref[:, cut(first_leaf + leaf)] = rows_all[g, h, :, cut(leaf)]

    def gram_pair(m, carry):
        for step in range(1, groups):
            rows_copy(m, step).wait_recv()
        for s in range(2):
            leaf = 2 * m + s
            everyone = rows_all[:, :, :, cut(leaf)].reshape(vecs * vec_dev, leaf_pts)
            gram_ref[first_leaf + leaf] = nt(rows_all[g, h, :, cut(leaf)], everyone) * (1.0 / leaf_pts)
            gram_out[leaf] = nt(rows_all[g, 1 - h, :, cut(leaf)], everyone) * (1.0 / leaf_pts)
        return carry

    lax.fori_loop(0, half_parents, gram_pair, 0)
    gram_copy = remote(
        gram_out, gram_ref.at[pl.ds(first_leaf, half_leaves)], gram_send.at[0], gram_recv.at[0], partner
    )
    gram_copy.start()

    geo_copy().wait_send()
    geo_forward(from_mate, 0).wait_send()
    own_forward().wait_send()
    settle(chunks(1, CHUNKS), sam_send.at[0], sam_frecv.at[0]).wait_send()
    settle(chunks(1, CHUNKS), sam_fsend.at[0], sam_frecv.at[0]).wait_send()

    @pl.when(gets_relay if GEO_DIRECT else sends_on)
    def _():
        geo_relay().wait_send()

    @pl.when(sends_on)
    def _():
        settle(chunks(1, RELAYED), sam_send.at[1], sam_frecv.at[0]).wait_send()

    @pl.when(gets_relay)
    def _():
        settle(chunks(1, DIRECT), sam_send.at[2], sam_frecv.at[0]).wait_send()
        geo_forward(from_relay, 1).wait_send()
        settle(chunks(1, CHUNKS), sam_fsend.at[1], sam_frecv.at[0]).wait_send()

    settle(coef_pk.at[pl.ds(0, columns), :, h], mate_send.at[0], coef_frecv.at[0]).wait_send()
    settle(coef_pk.at[:, :, h], coef_fsend.at[0], coef_frecv.at[0]).wait_send()
    settle(coef_pk.at[pl.ds(0, columns - 1), :, h], coef_send.at[0], coef_frecv.at[0]).wait_send()
    for step in range(1, groups):
        settle(rows_all.at[g], rows_send.at[step - 1], coef_frecv.at[0]).wait_send()
    settle(rows_all.at[g, 1 - h], out_send.at[0], out_recv.at[0]).wait_send()
    theirs = pl.ds(pl.multiple_of((1 - h) * half_leaves * leaf_pts, half_leaves * leaf_pts), half_leaves * leaf_pts)
    settle(out_ref.at[:, theirs], out_send.at[0], out_recv.at[0]).wait_recv()
    gram_copy.wait()


def write_kernel(out_ref, gram_ref, out_hbm, gram_hbm, sem):
    copies = [
        pltpu.make_async_copy(out_ref, out_hbm, sem.at[0]),
        pltpu.make_async_copy(gram_ref, gram_hbm, sem.at[1]),
    ]
    for copy in copies:
        copy.start()
    for copy in copies:
        copy.wait()


def per_device(
    samples, coords, panel_area, quad_weight, leaf_basis, transfer,
    coupling_fine, coupling_coarse, near_list, send_fine, send_coarse, far_fine, far_coarse,
):
    vec_dev, points = samples.shape
    leaf_dev, basis_rank, leaf_pts = leaf_basis.shape
    parents, half = leaf_dev // 2, leaf_dev // 2
    devices, vecs = lax.axis_size("leaf"), lax.axis_size("vec")
    groups, both = vecs // 2, 2 * vec_dev
    nb, nbc = coupling_fine.shape[1], coupling_coarse.shape[1]
    vmem = pl.BlockSpec(memory_space=pltpu.VMEM)
    hbm = pl.BlockSpec(memory_space=pl.ANY)
    bf16, f32 = jnp.bfloat16, jnp.float32
    dma = pltpu.SemaphoreType.DMA
    sample_out, gram = pl.pallas_call(
        main_kernel,
        out_shape=(
            pltpu.VMEM((vec_dev, points), bf16),
            pltpu.VMEM((leaf_dev, vec_dev, vecs * vec_dev), f32),
        ),
        in_specs=[hbm] * 13,
        out_specs=(vmem, vmem),
        scratch_shapes=[
            pltpu.SMEM(near_list.shape, jnp.int32),
            pltpu.SMEM(far_fine.shape, jnp.int32),
            pltpu.SMEM(far_coarse.shape, jnp.int32),
            pltpu.VMEM(coords.shape, f32),
            pltpu.VMEM((1, points), f32),
            pltpu.VMEM((1, points), f32),
            pltpu.VMEM(samples.shape, bf16),
            pltpu.VMEM(send_fine.shape, jnp.int32),
            pltpu.VMEM(send_coarse.shape, jnp.int32),
            pltpu.VMEM(transfer.shape, bf16),
            pltpu.VMEM(leaf_basis.shape, bf16),
            pltpu.VMEM((3 * leaf_dev, 4, leaf_pts), f32),
            pltpu.VMEM((3 * leaf_dev, 2, vec_dev, leaf_pts), bf16),
            pltpu.VMEM((devices, 2, 128), jnp.int32),
            pltpu.VMEM((devices, 2, 128), jnp.int32),
            pltpu.SMEM((devices, 2, 128), jnp.int32),
            pltpu.VMEM((devices, parents + parents // 2, 2, vec_dev, 2 * basis_rank), bf16),
            pltpu.VMEM((devices * leaf_dev, both, 2 * basis_rank), bf16),
            pltpu.VMEM((devices * parents, both, 2 * basis_rank), bf16),
            pltpu.VMEM((half, nb, basis_rank, basis_rank), bf16),
            pltpu.VMEM((half // 2, nbc, basis_rank, basis_rank), bf16),
            pltpu.VMEM((half, nb // 2, basis_rank, 2 * basis_rank), bf16),
            pltpu.VMEM((half // 2, nbc // 2, basis_rank, 2 * basis_rank), bf16),
            pltpu.VMEM((3 * leaf_dev, leaf_pts, 48), bf16),
            pltpu.VMEM((2, half, 48, leaf_pts), bf16),
            pltpu.VMEM((2, half, both, leaf_pts), f32),
            pltpu.VMEM((half, both, basis_rank), bf16),
            pltpu.VMEM((groups, 2, vec_dev, half * leaf_pts), bf16),
            pltpu.VMEM((half, vec_dev, vecs * vec_dev), f32),
            dma((2,)), dma((2,)), dma((2,)), dma((2,)),
            dma((3,)), dma((2, CHUNKS)), dma((2,)), dma((2,)), dma((1,)), dma((1,)),
            dma((1,)), dma((1,)),
            dma((1,)), dma((devices // 2,)), dma((1,)), dma((devices // 2,)),
            dma((1,)), dma((1,)),
            dma((groups - 1,)), dma((groups - 1, half // 2)),
            dma((1,)), dma((1,)),
            dma((1,)), dma((1,)),
            dma((14,)),
        ],
        compiler_params=pltpu.CompilerParams(
            vmem_limit_bytes=56 * 1024 * 1024, collective_id=0, has_side_effects=True
        ),
    )(
        near_list, far_fine, far_coarse,
        coords, panel_area[None, :], quad_weight[None, :], samples, send_fine, send_coarse,
        transfer, leaf_basis, coupling_fine, coupling_coarse,
    )
    return pl.pallas_call(
        write_kernel,
        out_shape=(
            jax.ShapeDtypeStruct(sample_out.shape, bf16),
            jax.ShapeDtypeStruct(gram.shape, f32),
        ),
        in_specs=[vmem] * 2,
        out_specs=(hbm, hbm),
        scratch_shapes=[dma((2,))],
    )(pltpu.with_memory_space_constraint(sample_out, pltpu.VMEM), pltpu.with_memory_space_constraint(gram, pltpu.VMEM))


def solution(mesh):
    return jax.shard_map(
        per_device,
        mesh=mesh,
        in_specs=(
            P("vec", "leaf"), P(None, "leaf"), P("leaf"), P("leaf"),
            P("leaf", None, None), P("leaf", None, None, None),
            P("leaf", None, None, None), P("leaf", None, None, None),
            P("leaf", None), P("leaf", None), P("leaf", None), P("leaf", None), P("leaf", None),
        ),
        out_specs=(P("vec", "leaf"), P("leaf", "vec", None)),
        check_vma=False,
    )
```

```python
import functools
import jax
import jax.numpy as jnp
from jax import lax
from jax.experimental import pallas as pl
from jax.experimental.pallas import tpu as pltpu
from jax.sharding import PartitionSpec as P

four_pi = 4.0 * 3.141592653589793
NT = (((1,), (1,)), ((), ()))
MESH = pl.DeviceIdType.MESH
LAG = 6
CHUNKS = 8
DIRECT = 2
GEO_DIRECT = False
RELAYED = CHUNKS - DIRECT
MATE_AT, FAR_AT = 1, 2


def pieces(block):
    first = block.astype(jnp.bfloat16).astype(jnp.float32)
    rest = block - first
    second = rest.astype(jnp.bfloat16).astype(jnp.float32)
    return first, second, rest - second


def main_kernel(
    near_hbm, farf_hbm, farc_hbm,
    coords_hbm, area_hbm, weight_hbm, sam_hbm, sendf_hbm, sendc_hbm, transfer_hbm, basis_hbm, cf_hbm, cc_hbm,
    out_ref, gram_ref,
    near_ref, farf_ref, farc_ref,
    coords_ref, area_ref, weight_ref, sam_ref, sendf_ref, sendc_ref, transfer_ref, basis_ref,
    geo_all, wvec, table, got, got_smem, coef_pk, fine_tab, coarse_tab, cf_ref, cc_ref, cf_pair, cc_pair,
    yfeat, xfeat, near_all, local_ref, rows_all, gram_out,
    geo_send, geo_recv, geo_fsend, geo_frecv, sam_send, sam_recv, sam_fsend, sam_frecv, own_send, own_recv,
    table_send, table_recv, coef_send, coef_recv, mate_send, mate_recv, coef_fsend, coef_frecv,
    rows_send, rows_recv, out_send, out_recv, gram_send, gram_recv, local_sem,
):
    leaf_dev, basis_rank, leaf_pts = basis_ref.shape
    vec_dev = sam_ref.shape[0]
    parents = leaf_dev // 2
    cap0, cap1 = sendf_ref.shape[1], sendc_ref.shape[1]
    nb = farf_ref.shape[1]
    nbc = farc_ref.shape[1]
    nn = near_ref.shape[1]
    half_leaves, half_parents = leaf_dev // 2, parents // 2
    both = 2 * vec_dev
    chunk = leaf_dev // CHUNKS
    devices, vecs = lax.axis_size("leaf"), lax.axis_size("vec")
    groups, columns = vecs // 2, devices // 2
    me, row = lax.axis_index("leaf"), lax.axis_index("vec")
    h, g = lax.rem(row, 2), lax.div(row, 2)
    partner = {"vec": row + 1 - 2 * h}
    first_leaf, first_parent = h * half_leaves, h * half_parents

    def leaf_peer(step):
        return {"leaf": lax.rem(me + step, devices)}

    def group_peer(step):
        return {"vec": lax.rem(g + step, groups) * 2 + h}

    def remote(src, dst, send, recv, peer):
        return pltpu.make_async_remote_copy(
            src_ref=src, dst_ref=dst, send_sem=send, recv_sem=recv,
            device_id=peer, device_id_type=MESH,
        )

    def cut(leaf):
        return pl.ds(pl.multiple_of(leaf * leaf_pts, leaf_pts), leaf_pts)

    def nt(a, b):
        return lax.dot_general(a, b, NT, preferred_element_type=jnp.float32)

    loads = [
        pltpu.make_async_copy(src, dst, local_sem.at[n])
        for n, (src, dst) in enumerate([
            (coords_hbm, coords_ref), (area_hbm, area_ref), (weight_hbm, weight_ref), (sam_hbm, sam_ref),
            (sendf_hbm, sendf_ref), (sendc_hbm, sendc_ref), (basis_hbm, basis_ref), (transfer_hbm, transfer_ref),
            (cf_hbm.at[pl.ds(first_leaf, half_leaves)], cf_ref),
            (cc_hbm.at[pl.ds(first_parent, half_parents)], cc_ref),
            (near_hbm, near_ref), (farf_hbm, farf_ref), (farc_hbm, farc_ref),
        ])
    ]
    for load in loads:
        load.start()
    barrier = pltpu.get_barrier_semaphore()

    def greet(step, carry):
        pl.semaphore_signal(barrier, inc=1, device_id=leaf_peer(step), device_id_type=MESH)
        return carry

    lax.fori_loop(1, devices, greet, 0)
    pl.semaphore_signal(barrier, inc=1, device_id=partner, device_id_type=MESH)
    for step in range(1, groups):
        pl.semaphore_signal(barrier, inc=1, device_id=group_peer(step), device_id_type=MESH)

    for load in loads[:6]:
        load.wait()

    def own(leaf, carry):
        xyz = coords_ref[:, cut(leaf)]
        norm = jnp.sum(xyz * xyz, axis=0, keepdims=True) + area_ref[:, cut(leaf)]
        geo_all[leaf_dev + leaf] = jnp.concatenate([xyz, norm], axis=0)
        weight = weight_ref[:, cut(leaf)] * (1.0 / four_pi)
        scaled = sam_ref[:, cut(leaf)].astype(jnp.float32) * weight
        wvec[leaf_dev + leaf, h] = scaled.astype(jnp.bfloat16)
        return carry

    lax.fori_loop(0, leaf_dev, own, 0, unroll=4)
    table[...] = jnp.zeros_like(table)

    def fill(d, carry):
        table[d, 0:1, 0:cap0] = sendf_ref[pl.ds(d, 1), :]
        table[d, 1:2, 0:cap1] = sendc_ref[pl.ds(d, 1), :]
        return carry

    lax.fori_loop(0, devices, fill, 0)
    got[me] = table[me]
    pl.semaphore_wait(barrier, devices - 1 + 1 + groups - 1)

    odd = lax.rem(me, 2)
    mate = {"leaf": me + 1 - 2 * odd}
    from_mate, from_relay = 2 * (1 - odd), 2 * odd
    onward = {"leaf": me + 2 - 4 * odd}
    other = {"leaf": me - 1 + 2 * odd}
    sends_on = jnp.where(odd == 0, me + 2 < devices, me >= 2)
    gets_relay = jnp.where(odd == 0, me >= 2, me + 2 < devices)

    def geo_part(part):
        return geo_all.at[pl.ds(part * leaf_dev + first_leaf, half_leaves)]

    def sam_part(part, c):
        return wvec.at[pl.ds(part * leaf_dev + c * chunk, chunk), h]

    def geo_copy():
        return remote(geo_part(1), geo_part(from_relay), geo_send.at[0], geo_recv.at[0], mate)

    def geo_relay():
        if GEO_DIRECT:
            return remote(geo_part(1), geo_part(from_mate), geo_send.at[1], geo_recv.at[1], other)
        return remote(geo_part(from_mate), geo_part(from_relay), geo_send.at[1], geo_recv.at[1], onward)

    def geo_forward(part, n):
        return remote(geo_part(part), geo_part(part), geo_fsend.at[n], geo_frecv.at[n], partner)

    def sam_copy(c):
        return remote(sam_part(1, c), sam_part(from_relay, c), sam_send.at[0], sam_recv.at[0, c], mate)

    def sam_relay(c):
        return remote(sam_part(from_mate, c), sam_part(from_relay, c), sam_send.at[1], sam_recv.at[1, c], onward)

    def sam_direct(c):
        return remote(sam_part(1, c), sam_part(from_mate, c), sam_send.at[2], sam_recv.at[1, c], other)

    def sam_forward(part, n, c):
        block = sam_part(part, c)
        return remote(block, block, sam_fsend.at[n], sam_frecv.at[n], partner)

    def settle(ref, send, recv):
        return remote(ref, ref, send, recv, partner)

    def chunks(part, count):
        return wvec.at[pl.ds(part * leaf_dev, count * chunk), h]

    def own_forward():
        block = wvec.at[pl.ds(leaf_dev, leaf_dev), h]
        return remote(block, block, own_send.at[0], own_recv.at[0], partner)

    def table_copy(step):
        peer = lax.rem(me + step, devices)
        return remote(table.at[peer], got.at[me], table_send.at[0], table_recv.at[0], {"leaf": peer})

    def same(step):
        return lax.rem(me + 2 * step, devices)

    def block_from(step):
        return lax.rem(me - 2 * step + devices, devices)

    def mate_block(step):
        return lax.rem(me + 1 - 2 * odd - 2 * step + devices, devices)

    def coef_copy(step):
        part = coef_pk.at[me, :, h]
        return remote(part, part, coef_send.at[0], coef_recv.at[step], {"leaf": same(step)})

    def coef_across(step):
        part = coef_pk.at[block_from(step), :, h]
        return remote(part, part, mate_send.at[0], mate_recv.at[step], mate)

    def coef_forward(step):
        part = coef_pk.at[block_from(step), :, h]
        return remote(part, part, coef_fsend.at[0], coef_frecv.at[0], partner)

    def mate_forward(step):
        part = coef_pk.at[mate_block(step), :, h]
        return remote(part, part, coef_fsend.at[0], coef_frecv.at[0], partner)

    geo_copy().start()
    if GEO_DIRECT:

        @pl.when(gets_relay)
        def _():
            geo_relay().start()

    sam_copy(0).start()

    @pl.when(gets_relay)
    def _():
        for c in range(RELAYED, CHUNKS):
            sam_direct(c).start()

    for c in range(1, CHUNKS):
        sam_copy(c).start()
    own_forward().start()

    def start_table(step, carry):
        table_copy(step).start()
        return carry

    lax.fori_loop(1, devices, start_table, 0)

    loads[6].wait()
    loads[7].wait()
    blank = jnp.zeros((basis_rank, leaf_pts), jnp.bfloat16)
    packed = []
    for m in range(parents):
        left = jnp.concatenate([basis_ref[2 * m], blank], axis=0)
        right = jnp.concatenate([blank, basis_ref[2 * m + 1]], axis=0)
        coef = nt(sam_ref[:, cut(2 * m)], left) + nt(sam_ref[:, cut(2 * m + 1)], right)
        coef = coef.astype(jnp.bfloat16)
        coef_pk[me, m, h] = coef
        packed.append(coef)
    coarse = []
    for m in range(parents):
        both_children = transfer_ref[m].reshape(2 * basis_rank, basis_rank)
        coarse.append(jnp.dot(packed[m], both_children, preferred_element_type=jnp.float32))
    for m in range(half_parents):
        pair = jnp.concatenate([coarse[2 * m], coarse[2 * m + 1]], axis=1)
        coef_pk[me, parents + m, h] = pair.astype(jnp.bfloat16)

    def start_coef(step, carry):
        coef_copy(step).start()
        return carry

    lax.fori_loop(1, columns, start_coef, 0)
    coef_across(0).start()
    coef_forward(0).start()

    def prepare(part):
        def source(leaf, carry):
            geo = geo_all[part * leaf_dev + leaf]
            ones = jnp.ones((1, leaf_pts), jnp.float32)
            rows = jnp.concatenate([geo, ones, jnp.zeros((3, leaf_pts), jnp.float32)], axis=0)
            y1, y2, y3 = pieces(rows)
            rows = jnp.concatenate([y1, y1, y1, y2, y2, y3], axis=0)
            yfeat[part * leaf_dev + leaf] = rows.T.astype(jnp.bfloat16)
            return carry

        lax.fori_loop(0, leaf_dev, source, 0, unroll=4)

    prepare(1)

    def target(leaf, carry):
        xyz = geo_all[leaf_dev + first_leaf + leaf][0:3]
        norm = jnp.sum(xyz * xyz, axis=0, keepdims=True)
        x8 = jnp.concatenate(
            [-2.0 * xyz, jnp.ones_like(norm), norm, jnp.zeros_like(xyz)], axis=0
        )
        x1, x2, x3 = pieces(x8)
        features = jnp.concatenate([x1, x2, x3, x1, x2, x1], axis=0).astype(jnp.bfloat16)
        xfeat[0, leaf] = features
        xfeat[1, leaf] = features
        return carry

    lax.fori_loop(0, half_leaves, target, 0, unroll=2)

    def pass_coef(step, carry):
        coef_copy(step).wait_recv()
        coef_across(step).start()
        coef_forward(step).start()
        return carry

    def pass_mate_sam(c):
        sam_copy(c).wait_recv()

        if c < RELAYED:

            @pl.when(sends_on)
            def _():
                sam_relay(c).start()

        sam_forward(from_mate, 0, c).start()

    geo_copy().wait_recv()

    if not GEO_DIRECT:

        @pl.when(sends_on)
        def _():
            geo_relay().start()

    geo_forward(from_mate, 0).start()
    pass_mate_sam(0)
    geo_forward(from_mate, 0).wait_recv()
    prepare(from_mate)
    for c in range(1, CHUNKS):
        pass_mate_sam(c)
    lax.fori_loop(1, columns, pass_coef, 0)

    loads[8].wait()
    loads[9].wait()

    def pair_up(src, dst):
        def one(i, carry):
            for b in range(src.shape[1] // 2):
                dst[i, b] = jnp.concatenate([src[i, 2 * b], src[i, 2 * b + 1]], axis=1)
            return carry

        lax.fori_loop(0, src.shape[0], one, 0, unroll=2)

    @pl.when(gets_relay)
    def _():
        geo_relay().wait_recv()
        geo_forward(from_relay, 1).start()

    pair_up(cf_ref, cf_pair)
    pair_up(cc_ref, cc_pair)

    @pl.when(gets_relay)
    def _():
        geo_forward(from_relay, 1).wait_recv()
        prepare(from_relay)
        for c in range(CHUNKS):
            sam_relay(c).wait_recv()
            sam_forward(from_relay, 1, c).start()

    own_forward().wait_recv()
    settle(chunks(from_mate, CHUNKS), sam_fsend.at[0], sam_frecv.at[0]).wait_recv()

    @pl.when(gets_relay)
    def _():
        settle(chunks(from_relay, CHUNKS), sam_fsend.at[1], sam_frecv.at[1]).wait_recv()

    loads[10].wait()

    def near_pair(m):
        base = (me - 1) * leaf_dev
        work = [(s, n) for s in range(2) for n in range(nn)]
        picked = [
            jnp.clip(near_ref[first_leaf + 2 * m + s, n] - base, 0, 3 * leaf_dev - 1) for s, n in work
        ]
        totals, dists = {}, {}
        for step in range(len(work) + LAG):
            if step < len(work):
                s, n = work[step]
                features = xfeat[n % 2, 2 * m + s]
                dists[step] = jnp.dot(yfeat[picked[step]], features, preferred_element_type=jnp.float32)
            if step >= LAG:
                s, n = work[step - LAG]
                block = lax.rsqrt(dists.pop(step - LAG).astype(jnp.bfloat16))
                values = wvec[picked[step - LAG]].reshape(both, leaf_pts)
                term = jnp.dot(values, block, preferred_element_type=jnp.float32)
                totals[s, n % 2] = term if n < 2 else totals[s, n % 2] + term
        for (s, lane), total in totals.items():
            near_all[lane, 2 * m + s] = total

    def pass_mate(step, carry):
        coef_across(step).wait_recv()
        mate_forward(step).start()
        return carry

    left_lanes = lax.broadcasted_iota(jnp.int32, (both, 2 * basis_rank), 1) < basis_rank

    def split(slot, cap):
        if cap & (cap - 1):
            return lax.div(slot, cap), lax.rem(slot, cap)
        return slot >> (cap.bit_length() - 1), slot & (cap - 1)

    def pair_term(tab, tiles, far_ref, at, cap, line, per_device, b):
        rows = []
        for lane in range(2):
            slot = far_ref[at, 2 * b + lane]
            source, place = split(slot, cap)
            index = source * per_device + got_smem[source, line, place]
            rows.append(tab[index ^ lane])
        return nt(jnp.where(left_lanes, rows[0], rows[1]), tiles[b])

    def fine_term(leaf, b):
        return pair_term(fine_tab, cf_pair.at[leaf], farf_ref, first_leaf + leaf, cap0, 0, leaf_dev, b)

    def coarse_term(m, b):
        return pair_term(coarse_tab, cc_pair.at[m], farc_ref, first_parent + m, cap1, 1, parents, b)

    def rows_copy(m, step):
        part = rows_all.at[g, :, :, pl.ds(pl.multiple_of(m * 2 * leaf_pts, 2 * leaf_pts), 2 * leaf_pts)]
        return remote(part, part, rows_send.at[step - 1], rows_recv.at[step - 1, m], group_peer(step))

    def out_copy(m):
        columns = pl.ds(pl.multiple_of(m * 2 * leaf_pts, 2 * leaf_pts), 2 * leaf_pts)
        start = (first_leaf + 2 * m) * leaf_pts
        there = pl.ds(pl.multiple_of(start, 2 * leaf_pts), 2 * leaf_pts)
        return remote(
            rows_all.at[g, 1 - h, :, columns], out_ref.at[:, there], out_send.at[0], out_recv.at[0], partner
        )

    def far_field():
        settle(got.at[pl.ds(0, devices - 1)], table_send.at[0], table_recv.at[0]).wait()
        settle(coef_pk.at[:, :, 1 - h], coef_fsend.at[0], coef_frecv.at[0]).wait_recv()
        to_smem = pltpu.make_async_copy(got, got_smem, local_sem.at[13])
        to_smem.start()

        def unpack(d, carry):
            for tab, count, first in ((fine_tab, parents, 0), (coarse_tab, half_parents, parents)):
                for m in range(count):
                    pair = coef_pk[d, first + m].reshape(both, 2 * basis_rank)
                    tab[2 * (d * count + m)] = pair
                    tab[2 * (d * count + m) + 1] = jnp.concatenate(
                        [pair[:, basis_rank:], pair[:, :basis_rank]], axis=1
                    )
            return carry

        lax.fori_loop(0, devices, unpack, 0, unroll=4)
        loads[11].wait()
        loads[12].wait()
        to_smem.wait()
        coarse_field = []
        for m in range(half_parents):
            field = coarse_term(m, 0)
            for b in range(1, nbc // 2):
                field = field + coarse_term(m, b)
            coarse_field.append(field.astype(jnp.bfloat16))
        for leaf in range(half_leaves):
            field = fine_term(leaf, 0)
            for b in range(1, nb // 2):
                field = field + fine_term(leaf, b)
            field = field + nt(coarse_field[leaf // 2], transfer_ref[first_parent + leaf // 2, leaf % 2])
            local_ref[leaf] = field.astype(jnp.bfloat16)

    def emit(m):
        for s in range(2):
            leaf = 2 * m + s
            far = jnp.dot(local_ref[leaf], basis_ref[first_leaf + leaf], preferred_element_type=jnp.float32)
            result = (near_all[0, leaf] + near_all[1, leaf] + far).astype(out_ref.dtype)
            result = result.reshape(2, vec_dev, leaf_pts)
            rows_all[g, :, :, cut(leaf)] = result
        for step in range(1, groups):
            rows_copy(m, step).start()
        out_copy(m).start()

    def near_step(m, carry):
        near_pair(m)

        @pl.when(m == MATE_AT)
        def _():
            lax.fori_loop(0, columns, pass_mate, 0)

        @pl.when(m == FAR_AT)
        def _():
            far_field()
            for done in range(FAR_AT):
                emit(done)

        @pl.when(m >= FAR_AT)
        def _():
            emit(m)
        return carry

    lax.fori_loop(0, half_parents, near_step, 0)

    for leaf in range(half_leaves):
        out_ref[:, cut(first_leaf + leaf)] = rows_all[g, h, :, cut(leaf)]

    def gram_pair(m, carry):
        for step in range(1, groups):
            rows_copy(m, step).wait_recv()
        for s in range(2):
            leaf = 2 * m + s
            everyone = rows_all[:, :, :, cut(leaf)].reshape(vecs * vec_dev, leaf_pts)
            gram_ref[first_leaf + leaf] = nt(rows_all[g, h, :, cut(leaf)], everyone) * (1.0 / leaf_pts)
            gram_out[leaf] = nt(rows_all[g, 1 - h, :, cut(leaf)], everyone) * (1.0 / leaf_pts)
        return carry

    lax.fori_loop(0, half_parents, gram_pair, 0)
    gram_copy = remote(
        gram_out, gram_ref.at[pl.ds(first_leaf, half_leaves)], gram_send.at[0], gram_recv.at[0], partner
    )
    gram_copy.start()

    geo_copy().wait_send()
    geo_forward(from_mate, 0).wait_send()
    own_forward().wait_send()
    settle(chunks(1, CHUNKS), sam_send.at[0], sam_frecv.at[0]).wait_send()
    settle(chunks(1, CHUNKS), sam_fsend.at[0], sam_frecv.at[0]).wait_send()

    @pl.when(gets_relay if GEO_DIRECT else sends_on)
    def _():
        geo_relay().wait_send()

    @pl.when(sends_on)
    def _():
        settle(chunks(1, RELAYED), sam_send.at[1], sam_frecv.at[0]).wait_send()

    @pl.when(gets_relay)
    def _():
        settle(chunks(1, DIRECT), sam_send.at[2], sam_frecv.at[0]).wait_send()
        geo_forward(from_relay, 1).wait_send()
        settle(chunks(1, CHUNKS), sam_fsend.at[1], sam_frecv.at[0]).wait_send()

    settle(coef_pk.at[pl.ds(0, columns), :, h], mate_send.at[0], coef_frecv.at[0]).wait_send()
    settle(coef_pk.at[:, :, h], coef_fsend.at[0], coef_frecv.at[0]).wait_send()
    settle(coef_pk.at[pl.ds(0, columns - 1), :, h], coef_send.at[0], coef_frecv.at[0]).wait_send()
    for step in range(1, groups):
        settle(rows_all.at[g], rows_send.at[step - 1], coef_frecv.at[0]).wait_send()
    settle(rows_all.at[g, 1 - h], out_send.at[0], out_recv.at[0]).wait_send()
    theirs = pl.ds(pl.multiple_of((1 - h) * half_leaves * leaf_pts, half_leaves * leaf_pts), half_leaves * leaf_pts)
    settle(out_ref.at[:, theirs], out_send.at[0], out_recv.at[0]).wait_recv()
    gram_copy.wait()


def write_kernel(out_ref, gram_ref, out_hbm, gram_hbm, sem):
    copies = [
        pltpu.make_async_copy(out_ref, out_hbm, sem.at[0]),
        pltpu.make_async_copy(gram_ref, gram_hbm, sem.at[1]),
    ]
    for copy in copies:
        copy.start()
    for copy in copies:
        copy.wait()


def per_device(
    samples, coords, panel_area, quad_weight, leaf_basis, transfer,
    coupling_fine, coupling_coarse, near_list, send_fine, send_coarse, far_fine, far_coarse,
):
    vec_dev, points = samples.shape
    leaf_dev, basis_rank, leaf_pts = leaf_basis.shape
    parents, half = leaf_dev // 2, leaf_dev // 2
    devices, vecs = lax.axis_size("leaf"), lax.axis_size("vec")
    groups, both = vecs // 2, 2 * vec_dev
    nb, nbc = coupling_fine.shape[1], coupling_coarse.shape[1]
    vmem = pl.BlockSpec(memory_space=pltpu.VMEM)
    hbm = pl.BlockSpec(memory_space=pl.ANY)
    bf16, f32 = jnp.bfloat16, jnp.float32
    dma = pltpu.SemaphoreType.DMA
    sample_out, gram = pl.pallas_call(
        main_kernel,
        out_shape=(
            pltpu.VMEM((vec_dev, points), bf16),
            pltpu.VMEM((leaf_dev, vec_dev, vecs * vec_dev), f32),
        ),
        in_specs=[hbm] * 13,
        out_specs=(vmem, vmem),
        scratch_shapes=[
            pltpu.SMEM(near_list.shape, jnp.int32),
            pltpu.SMEM(far_fine.shape, jnp.int32),
            pltpu.SMEM(far_coarse.shape, jnp.int32),
            pltpu.VMEM(coords.shape, f32),
            pltpu.VMEM((1, points), f32),
            pltpu.VMEM((1, points), f32),
            pltpu.VMEM(samples.shape, bf16),
            pltpu.VMEM(send_fine.shape, jnp.int32),
            pltpu.VMEM(send_coarse.shape, jnp.int32),
            pltpu.VMEM(transfer.shape, bf16),
            pltpu.VMEM(leaf_basis.shape, bf16),
            pltpu.VMEM((3 * leaf_dev, 4, leaf_pts), f32),
            pltpu.VMEM((3 * leaf_dev, 2, vec_dev, leaf_pts), bf16),
            pltpu.VMEM((devices, 2, 128), jnp.int32),
            pltpu.VMEM((devices, 2, 128), jnp.int32),
            pltpu.SMEM((devices, 2, 128), jnp.int32),
            pltpu.VMEM((devices, parents + parents // 2, 2, vec_dev, 2 * basis_rank), bf16),
            pltpu.VMEM((devices * leaf_dev, both, 2 * basis_rank), bf16),
            pltpu.VMEM((devices * parents, both, 2 * basis_rank), bf16),
            pltpu.VMEM((half, nb, basis_rank, basis_rank), bf16),
            pltpu.VMEM((half // 2, nbc, basis_rank, basis_rank), bf16),
            pltpu.VMEM((half, nb // 2, basis_rank, 2 * basis_rank), bf16),
            pltpu.VMEM((half // 2, nbc // 2, basis_rank, 2 * basis_rank), bf16),
            pltpu.VMEM((3 * leaf_dev, leaf_pts, 48), bf16),
            pltpu.VMEM((2, half, 48, leaf_pts), bf16),
            pltpu.VMEM((2, half, both, leaf_pts), f32),
            pltpu.VMEM((half, both, basis_rank), bf16),
            pltpu.VMEM((groups, 2, vec_dev, half * leaf_pts), bf16),
            pltpu.VMEM((half, vec_dev, vecs * vec_dev), f32),
            dma((2,)), dma((2,)), dma((2,)), dma((2,)),
            dma((3,)), dma((2, CHUNKS)), dma((2,)), dma((2,)), dma((1,)), dma((1,)),
            dma((1,)), dma((1,)),
            dma((1,)), dma((devices // 2,)), dma((1,)), dma((devices // 2,)),
            dma((1,)), dma((1,)),
            dma((groups - 1,)), dma((groups - 1, half // 2)),
            dma((1,)), dma((1,)),
            dma((1,)), dma((1,)),
            dma((14,)),
        ],
        compiler_params=pltpu.CompilerParams(
            vmem_limit_bytes=56 * 1024 * 1024, collective_id=0, has_side_effects=True
        ),
    )(
        near_list, far_fine, far_coarse,
        coords, panel_area[None, :], quad_weight[None, :], samples, send_fine, send_coarse,
        transfer, leaf_basis, coupling_fine, coupling_coarse,
    )
    return pl.pallas_call(
        write_kernel,
        out_shape=(
            jax.ShapeDtypeStruct(sample_out.shape, bf16),
            jax.ShapeDtypeStruct(gram.shape, f32),
        ),
        in_specs=[vmem] * 2,
        out_specs=(hbm, hbm),
        scratch_shapes=[dma((2,))],
    )(pltpu.with_memory_space_constraint(sample_out, pltpu.VMEM), pltpu.with_memory_space_constraint(gram, pltpu.VMEM))


def solution(mesh):
    return jax.shard_map(
        per_device,
        mesh=mesh,
        in_specs=(
            P("vec", "leaf"), P(None, "leaf"), P("leaf"), P("leaf"),
            P("leaf", None, None), P("leaf", None, None, None),
            P("leaf", None, None, None), P("leaf", None, None, None),
            P("leaf", None), P("leaf", None), P("leaf", None), P("leaf", None), P("leaf", None),
        ),
        out_specs=(P("vec", "leaf"), P("leaf", "vec", None)),
        check_vma=False,
    )
```
